128 devices in a mesh: rep: 1, r: 16 (over y, z), s: 8 (over x, core).
Axes of the slice: x: 4, y: 4, z: 4, core: 2. Of those that a mesh axis runs over, the one named last changes fastest.
Arguments:
- x: bfloat16 [128, 2048, 1024], P(('rep', 'r', 's'))
- dy: bfloat16 [128, 2048, 1024], P(('rep', 'r', 's'))
- w_gate: bfloat16 [2, 1024, 3328], P(None, 's')
- w_up: bfloat16 [2, 1024, 3328], P(None, 's')
- w_down: bfloat16 [2, 3328, 1024], P(None, 's')
- m_w_gate: float32 [2, 1024, 3328], P(None, 's')
- m_w_up: float32 [2, 1024, 3328], P(None, 's')
- m_w_down: float32 [2, 3328, 1024], P(None, 's')
- v_w_gate: float32 [2, 1024, 3328], P(None, 's')
- v_w_up: float32 [2, 1024, 3328], P(None, 's')
- v_w_down: float32 [2, 3328, 1024], P(None, 's')
Outputs:
- output 1: bfloat16 [2, 1024, 3328], P('rep', 's')
- output 2: bfloat16 [2, 1024, 3328], P('rep', 's')
- output 3: bfloat16 [2, 3328, 1024], P('rep', 's')
- output 4: float32 [2, 1024, 3328], P('rep', 's')
- output 5: float32 [2, 1024, 3328], P('rep', 's')
- output 6: float32 [2, 3328, 1024], P('rep', 's')
- output 7: float32 [2, 1024, 3328], P('rep', 's')
- output 8: float32 [2, 1024, 3328], P('rep', 's')
- output 9: float32 [2, 3328, 1024], P('rep', 's')
All inputs are finite; a program needn't handle non-finite values.
Results may differ from the reference program's by a relative error of at most 0.022.
Values are sent between devices in bfloat16 or wider.
A program may use at most 1.5 GiB of HBM per device.

```python
import jax
import jax.numpy as jnp
from jax import lax

SEQUENCES = 128
TOKENS = 2048
D = 1024
FF = 3328
LAYERS = 2
NAMES = ("w_gate", "w_up", "w_down")
SHAPES = {"w_gate": (LAYERS, D, FF), "w_up": (LAYERS, D, FF), "w_down": (LAYERS, FF, D)}


def bump(key, n, height):
    away = (jnp.arange(n, dtype=jnp.int32) - jax.random.randint(key, (), 0, n, jnp.int32)) % n
    return jnp.where(away < n // 8, height, 1.0)


def together(key, own, strength):
    shared = jax.random.normal(key, own.shape[1:], jnp.float32)
    return (own + strength * shared) * lax.rsqrt(1 + strength * strength)


def setup_inputs(seed: int = 0, part: int = 0) -> dict:
    kx, kdy, ka, kb, kz, kf, kh, kl, *keys = jax.random.split(jax.random.key(seed), 8 + 3 * len(NAMES))
    kx, kdy, ka, kb = (jax.random.fold_in(k, part) for k in (kx, kdy, ka, kb))
    kw, km, kv = (keys[i::3] for i in range(3))
    shape = (SEQUENCES, TOKENS, D)
    much_x, much_dy = jax.random.uniform(kz, (2,), jnp.float32, 0.0, 1.0)
    loud = 2.0 ** jax.random.uniform(jax.random.fold_in(kz, 1), (), jnp.float32, -1.0, 2.0)
    layers = 2.0 ** jax.random.uniform(kl, (LAYERS, 1, 1), jnp.float32, -1.0, 1.0)
    x = together(ka, jax.random.normal(kx, shape, jnp.float32), much_x) * bump(kf, D, 4.0)
    dy = together(kb, jax.random.normal(kdy, shape, jnp.float32), much_dy)
    drawn = {"x": x.astype(jnp.bfloat16), "dy": (loud * dy * (SEQUENCES * TOKENS) ** -0.5).astype(jnp.bfloat16)}
    for key, name in zip(kw, NAMES, strict=True):
        w = jax.random.normal(key, SHAPES[name], jnp.float32) * SHAPES[name][1] ** -0.5
        drawn[name] = (w * {"w_gate": 1.0, "w_up": bump(kh, FF, 4.0), "w_down": layers}[name]).astype(jnp.bfloat16)
    for key, name in zip(km, NAMES, strict=True):
        drawn[f"m_{name}"] = 0.1 * jax.random.normal(key, SHAPES[name], jnp.float32)
    for key, name in zip(kv, NAMES, strict=True):
        drawn[f"v_{name}"] = loud * loud * jax.random.uniform(key, SHAPES[name], jnp.float32, 0.05, 0.15)
    return drawn


def matmul(a, w):
    return jnp.dot(a, w, preferred_element_type=jnp.float32).astype(jnp.bfloat16)


def normed(h):
    wide = h.astype(jnp.float32)
    scale = lax.rsqrt(jnp.mean(wide**2, -1, keepdims=True) + 1e-6)
    return (wide * scale).astype(jnp.bfloat16)


def layer(h, w):
    a = normed(h)
    gate = jnp.dot(a, w["w_gate"], preferred_element_type=jnp.float32)
    up = jnp.dot(a, w["w_up"], preferred_element_type=jnp.float32)
    return h + matmul((jax.nn.silu(gate) * up).astype(jnp.bfloat16), w["w_down"])


def adamw(w, m, v, g):
    m = 0.9 * m + 0.1 * g
    v = 0.95 * v + 0.05 * g * g
    step = m * lax.rsqrt(v + 1e-8) + 0.1 * w
    return (w - 0.02 * step).astype(jnp.bfloat16), m, v


def stack(weights, h):
    return lax.scan(lambda h, w: (layer(h, w), None), h, weights)[0]


def reference(x, dy, w_gate, w_up, w_down, m_w_gate, m_w_up, m_w_down, v_w_gate, v_w_up, v_w_down):
    weights = dict(zip(NAMES, (w_gate, w_up, w_down), strict=True))

    def take(so_far, sequence):
        h, by_y = sequence
        _, back = jax.vjp(lambda w: stack(w, h), weights)
        return jax.tree.map(lambda total, term: total + term.astype(jnp.float32), so_far, back(by_y)[0]), None

    none_yet = {name: jnp.zeros(w.shape, jnp.float32) for name, w in weights.items()}
    by_weights, _ = lax.scan(take, none_yet, (x, dy))
    gradients = [by_weights[name].astype(jnp.bfloat16).astype(jnp.float32) for name in NAMES]
    new = [
        adamw(w.astype(jnp.float32), m, v, g)
        for w, m, v, g in zip((w_gate, w_up, w_down), (m_w_gate, m_w_up, m_w_down), (v_w_gate, v_w_up, v_w_down), gradients, strict=True)
    ]
    return tuple(one[which] for which in range(3) for one in new)
```

```python
import functools

import jax
import jax.numpy as jnp
from jax import lax
from jax.experimental import pallas as pl
from jax.experimental.pallas import tpu as pltpu
from jax.sharding import PartitionSpec as P

MESH = pl.DeviceIdType.MESH
f32, bf16 = jnp.float32, jnp.bfloat16
TN = 256
MC = 512
U = 128
VMEM_LIMIT = 62 * 2**20


def dot(a, b):
    return lax.dot_general(a, b, (((1,), (0,)), ((), ())), preferred_element_type=f32)


def dot_nt(a, b):
    return lax.dot_general(a, b, (((1,), (1,)), ((), ())), preferred_element_type=f32)


def normed(h):
    wide = h.astype(f32)
    scale = lax.rsqrt(jnp.mean(wide**2, -1, keepdims=True) + 1e-6)
    return (wide * scale).astype(bf16)


def chunks(n, step):
    return [pl.ds(i, step) for i in range(0, n, step)]


def forward_kernel(tiles, x_ref, wg_ref, wu_ref, wd_ref, s_ref, t_ref, p_ref, h_ref, a, acc):
    j = pl.program_id(0)
    tokens = x_ref.shape[0]

    @pl.when(j == 0)
    def _():
        for r in chunks(tokens, 256):
            a[r, :] = normed(x_ref[r, :])
            acc[r, :] = jnp.zeros_like(acc[r, :])

    for r in chunks(tokens, MC):
        g = dot(a[r, :], wg_ref[...])
        u = dot(a[r, :], wu_ref[...])
        sig = jax.nn.sigmoid(g)
        silu = g * sig
        s_ref[r, :] = silu
        t_ref[r, :] = u * (sig * (1 + g * (1 - sig)))
        p_ref[r, :] = (silu * u).astype(bf16)
    for r in chunks(tokens, MC):
        acc[r, :] += dot(p_ref[r, :], wd_ref[...])

    @pl.when(j == tiles - 1)
    def _():
        for r in chunks(tokens, 256):
            h_ref[r, :] = (x_ref[r, :].astype(f32) + acc[r, :].astype(bf16).astype(f32)).astype(bf16)


def forward(x, wg, wu, wd):
    tokens, d = x.shape
    ff = wg.shape[1]
    tiles = ff // TN
    whole = pl.BlockSpec((tokens, d), lambda j: (0, 0), pipeline_mode=pl.Buffered(1))
    cols = pl.BlockSpec((d, TN), lambda j: (0, j))
    hid = pl.BlockSpec((tokens, TN), lambda j: (0, j))
    return pl.pallas_call(
        functools.partial(forward_kernel, tiles),
        grid=(tiles,),
        in_specs=[whole, cols, cols, pl.BlockSpec((TN, d), lambda j: (j, 0))],
        out_specs=[hid, hid, hid, whole],
        out_shape=[jax.ShapeDtypeStruct((tokens, ff), f32)] * 2
        + [jax.ShapeDtypeStruct((tokens, ff), bf16), jax.ShapeDtypeStruct((tokens, d), bf16)],
        scratch_shapes=[pltpu.VMEM((tokens, d), bf16), pltpu.VMEM((tokens, d), f32)],
        compiler_params=pltpu.CompilerParams(vmem_limit_bytes=VMEM_LIMIT),
        cost_estimate=pl.CostEstimate(flops=6 * tokens * d * ff, bytes_accessed=10 * tokens * ff, transcendentals=0),
        name="forward0",
    )(x, wg, wu, wd)


def backward_kernel(tiles, x_ref, h_ref, dy_ref, wg_ref, wu_ref, wd1_ref, wd0_ref, s_ref, t_ref, p_ref,
                    ggu_ref, gwd_ref,
                    a, at, dy, accg, accu, pbuf, dg, du, dgu, dwd, r0gu, r0wd, s1, r1, s2, r2, s3, r3, fin,
                    lsem, s0s, s0r, s1s, s1r, s2s, s2r, s3s, s3r, ags, agr, ago):
    i = pl.program_id(0)
    tokens = a.shape[0]
    r, s = lax.axis_index("r"), lax.axis_index("s")
    y, z, xx, c = r // 4, r % 4, s // 2, s % 2
    total = 2 * tiles
    where = {"x": xx, "y": y, "z": z}
    ORDER = ("yzx", "zxy", "xyz")

    def to(dim, d):
        if dim == "y":
            return (0, lax.rem(y + d, 4) * 4 + z, s)
        if dim == "z":
            return (0, y * 4 + lax.rem(z + d, 4), s)
        return (0, r, lax.rem(xx + d, 4) * 2 + c)

    def remote(src, dst, ss, rs, dev):
        return pltpu.make_async_remote_copy(src_ref=src, dst_ref=dst, send_sem=ss, recv_sem=rs, device_id=dev, device_id_type=MESH)

    def stage0(tile):
        slot = lax.rem(tile, 2)
        peer = (0, r, s + 1 - 2 * c)
        return [
            remote(dgu.at[:, :, 1 - c], r0gu.at[slot], s0s.at[0], s0r.at[slot, 0], peer),
            remote(dwd.at[1 - c], r0wd.at[slot], s0s.at[1], s0r.at[slot, 1], peer),
        ]

    def exchange(n, src, dst, ss, rs, tile):
        slot = lax.rem(tile, 2)
        copies = []
        for q in range(3):
            dim = ORDER[q][n]
            for d in (1, 2, 3):
                copies.append(
                    remote(src.at[q, lax.rem(where[dim] + d, 4)], dst.at[slot, q, d - 1], ss.at[q, d - 1], rs.at[slot, q, d - 1], to(dim, d))
                )
        return copies

    stages = [functools.partial(exchange, n, *refs) for n, refs in enumerate(((s1, r1, s1s, s1r), (s2, r2, s2s, s2r), (s3, r3, s3s, s3r)))]

    def added(n, src, dst, tile, q):
        slot = lax.rem(tile, 2)
        own = src[q, where[ORDER[q][n]]].astype(f32)
        return (own + dst[slot, q, 0].astype(f32) + dst[slot, q, 1].astype(f32) + dst[slot, q, 2].astype(f32)).astype(bf16)

    def spread(tile, d):
        layer, j = 1 - tile // tiles, lax.rem(tile, tiles)
        to_r = lax.rem(r + d, 16)
        row = 16 * j + r
        owner = row // 26
        gu = (fin.at[tile, pl.ds(0, 2)], ggu_ref.at[layer, r, j])
        wd = (fin.at[tile, 2], gwd_ref.at[layer, row - 26 * owner, 4 * c + xx])
        return gu, wd, (0, to_r, s), (0, to_r, owner), owner

    def own_spread(tile, act):
        gu, wd, _, to_wd, owner = spread(tile, 0)
        if act == "start":
            pltpu.make_async_copy(*gu, agr.at[0]).start()

        @pl.when(owner == s)
        def _():
            if act == "start":
                pltpu.make_async_copy(*wd, agr.at[1]).start()

        @pl.when(owner != s)
        def _():
            cp = remote(*wd, ago.at[0], agr.at[1], to_wd)
            cp.start() if act == "start" else cp.wait_send()

    @pl.when(i == 0)
    def _():
        cp = [pltpu.make_async_copy(h_ref, a, lsem.at[0]), pltpu.make_async_copy(dy_ref, dy, lsem.at[1])]
        cp[0].start()
        cp[1].start()
        cp[0].wait()
        for rows in chunks(tokens, 256):
            v = normed(a[rows, :])
            a[rows, :] = v
            at[:, rows] = v.T
            accg[rows, :] = jnp.zeros_like(accg[rows, :])
            accu[rows, :] = jnp.zeros_like(accu[rows, :])
        cp[1].wait()

    @pl.when(i < tiles)
    def _():
        for rows in chunks(tokens, MC):
            g = dot(a[rows, :], wg_ref[...])
            u = dot(a[rows, :], wu_ref[...])
            d = dot_nt(dy[rows, :], wd1_ref[...]).astype(bf16).astype(f32)
            sig = jax.nn.sigmoid(g)
            silu = g * sig
            pbuf[rows, :] = (silu * u).astype(bf16)
            du[rows, :] = (d * silu).astype(bf16)
            dg[rows, :] = (d * u * (sig * (1 + g * (1 - sig)))).astype(bf16)
        for rows in chunks(tokens, MC):
            accg[rows, :] += dot_nt(dg[rows, :], wg_ref[...])
            accu[rows, :] += dot_nt(du[rows, :], wu_ref[...])

    @pl.when((i >= tiles) & (i < total))
    def _():
        for rows in chunks(tokens, MC):
            d = dot_nt(dy[rows, :], wd0_ref[...]).astype(bf16).astype(f32)
            du[rows, :] = (d * s_ref[rows, :]).astype(bf16)
            dg[rows, :] = (d * t_ref[rows, :]).astype(bf16)
            pbuf[rows, :] = p_ref[rows, :]

    @pl.when((i >= 4) & (i < total + 4))
    def _():
        tile = i - 4
        for cp in stages[2](tile):
            cp.wait()
        for q in range(3):
            fin[tile, q] = added(2, s3, r3, tile, q)
        own_spread(tile, "start")

        def send(d, _):
            gu, wd, to_gu, to_wd, _o = spread(tile, d)
            remote(*gu, ags.at[0], agr.at[0], to_gu).start()
            remote(*wd, ags.at[1], agr.at[1], to_wd).start()
            return 0

        lax.fori_loop(1, 16, send, 0)

    @pl.when((i >= 3) & (i < total + 3))
    def _():
        tile = i - 3
        for cp in stages[1](tile):
            cp.wait()
        for q in range(3):
            s3[q] = added(1, s2, r2, tile, q)
        for cp in stages[2](tile):
            cp.start()

    @pl.when((i >= 2) & (i < total + 2))
    def _():
        tile = i - 2
        for cp in stages[0](tile):
            cp.wait()
        for q in range(3):
            s2[q] = added(0, s1, r1, tile, q)
        for cp in stages[1](tile):
            cp.start()

    @pl.when((i >= 1) & (i < total + 1))
    def _():
        tile = i - 1
        slot = lax.rem(tile, 2)
        for cp in stage0(tile):
            cp.wait()
        for xi in range(4):
            for k in range(8):
                for h in range(2):
                    rows, cols = pl.ds(16 * k, 16), pl.ds(U * h, U)
                    yi, zi = k // 2, 2 * (k % 2) + h
                    for q, at_ in ((0, (yi, zi, xi)), (1, (zi, xi, yi))):
                        v = dgu[q, xi, c, rows, cols].astype(f32) + r0gu[slot, q, xi, rows, cols].astype(f32)
                        s1[(q, *at_)] = v.astype(bf16)
                    unit = 2 * k + h
                    rows, cols = pl.ds(16 * unit, 16), pl.ds(U * xi, U)
                    v = dwd[c, rows, cols].astype(f32) + r0wd[slot, rows, cols].astype(f32)
                    s1[2, xi, unit // 4, unit % 4] = v.astype(bf16)
        for cp in stages[0](tile):
            cp.start()

    @pl.when(i < total)
    def _():
        for q, one in ((0, dg), (1, du)):
            g = dot(at[...], one[...]).astype(bf16)
            dgu[q] = g.reshape(dgu.shape[1:])
        g = dot(pbuf[...].T, dy[...]).astype(bf16)
        dwd[0] = g[:, :512]
        dwd[1] = g[:, 512:]
        for cp in stage0(i):
            cp.start()

    @pl.when(i == tiles - 1)
    def _():
        cp = pltpu.make_async_copy(h_ref, a, lsem.at[0])
        cp.start()
        cp.wait()
        for rows in chunks(tokens, 256):
            da = (accg[rows, :].astype(bf16).astype(f32) + accu[rows, :].astype(bf16).astype(f32)).astype(bf16).astype(f32)
            wide = a[rows, :].astype(f32)
            scale = lax.rsqrt(jnp.mean(wide**2, -1, keepdims=True) + 1e-6)
            along = jnp.sum(da * wide, -1, keepdims=True)
            by_h = da * scale - wide * (along * (scale * scale * scale) * (1.0 / wide.shape[-1]))
            dy[rows, :] = (dy[rows, :].astype(f32) + by_h.astype(bf16).astype(f32)).astype(bf16)
        cp = pltpu.make_async_copy(x_ref, a, lsem.at[0])
        cp.start()
        cp.wait()
        for rows in chunks(tokens, 256):
            at[:, rows] = normed(a[rows, :]).T

    @pl.when(i == total + 3)
    def _():
        remote(ggu_ref.at[:, pl.ds(0, 15)], ggu_ref.at[:, pl.ds(0, 15)], ags.at[0], agr.at[0], to("y", 1)).wait_send()
        half = ggu_ref.at[0, pl.ds(0, 15)]
        remote(half, half, ags.at[1], agr.at[1], to("y", 1)).wait_send()

        def done(tile, _):
            own_spread(tile, "wait")
            return 0

        lax.fori_loop(0, total, done, 0)
        pltpu.make_async_copy(ggu_ref, ggu_ref, agr.at[0]).wait()
        pltpu.make_async_copy(gwd_ref, gwd_ref, agr.at[1]).wait()


def backward(x, h, dy, wg, wu, wd1, wd0, s, t, p):
    tokens, d = x.shape
    ff = wg.shape[1]
    tiles = ff // TN
    last = tiles - 1
    anywhere = pl.BlockSpec(memory_space=pl.ANY)
    cols = pl.BlockSpec((d, TN), lambda i: (0, jnp.minimum(i, last)))
    clamp = lambda i: jnp.clip(i - tiles, 0, last)
    hid = pl.BlockSpec((tokens, TN), lambda i: (0, clamp(i)))
    dma = pltpu.SemaphoreType.DMA
    unit = (16, U)
    return pl.pallas_call(
        functools.partial(backward_kernel, tiles),
        grid=(2 * tiles + 4,),
        in_specs=[anywhere] * 3
        + [cols, cols, pl.BlockSpec((TN, d), lambda i: (jnp.minimum(i, last), 0)), pl.BlockSpec((TN, d), lambda i: (clamp(i), 0))]
        + [hid] * 3,
        out_specs=[anywhere] * 2,
        out_shape=[jax.ShapeDtypeStruct((2, 16, tiles, 2, *unit), bf16), jax.ShapeDtypeStruct((2, 26, 8, *unit), bf16)],
        scratch_shapes=[
            pltpu.VMEM((tokens, d), bf16),
            pltpu.VMEM((d, tokens), bf16),
            pltpu.VMEM((tokens, d), bf16),
            pltpu.VMEM((tokens, d), f32),
            pltpu.VMEM((tokens, d), f32),
            pltpu.VMEM((tokens, TN), bf16),
            pltpu.VMEM((tokens, TN), bf16),
            pltpu.VMEM((tokens, TN), bf16),
            pltpu.VMEM((2, 4, 2, 128, TN), bf16),
            pltpu.VMEM((2, TN, 512), bf16),
            pltpu.VMEM((2, 2, 4, 128, TN), bf16),
            pltpu.VMEM((2, TN, 512), bf16),
            pltpu.VMEM((3, 4, 4, 4, *unit), bf16),
            pltpu.VMEM((2, 3, 3, 4, 4, *unit), bf16),
            pltpu.VMEM((3, 4, 4, *unit), bf16),
            pltpu.VMEM((2, 3, 3, 4, *unit), bf16),
            pltpu.VMEM((3, 4, *unit), bf16),
            pltpu.VMEM((2, 3, 3, *unit), bf16),
            pltpu.VMEM((2 * tiles, 3, *unit), bf16),
            dma((2,)),
            dma((2,)),
            dma((2, 2)),
        ]
        + [dma((3, 3)), dma((2, 3, 3))] * 3
        + [dma((2,)), dma((2,)), dma((1,))],
        compiler_params=pltpu.CompilerParams(vmem_limit_bytes=VMEM_LIMIT, has_side_effects=True),
        cost_estimate=pl.CostEstimate(flops=24 * tokens * d * ff, bytes_accessed=10 * tokens * ff, transcendentals=0),
        name="backward",
    )(x, h, dy, wg, wu, wd1, wd0, s, t, p)


def adamw(w, m, v, g):
    m = 0.9 * m + 0.1 * g
    v = 0.95 * v + 0.05 * g * g
    step = m * lax.rsqrt(v + 1e-8) + 0.1 * w
    return (w - 0.02 * step).astype(bf16), m, v


def update_kernel(ggu_ref, gwd_ref, *refs):
    ins, outs = refs[:9], refs[9:]
    for q in range(2):
        for k in range(8):
            for h in range(2):
                at_ = (0, pl.ds(16 * k, 16), pl.ds(U * h, U))
                new = adamw(ins[q][at_].astype(f32), ins[3 + q][at_], ins[6 + q][at_], ggu_ref[0, 2 * k + h, 0, q].astype(f32))
                for n, one in enumerate(new):
                    outs[3 * n + q][at_] = one
    for k in range(2):
        for h in range(8):
            at_ = (0, pl.ds(16 * k, 16), pl.ds(U * h, U))
            new = adamw(ins[2][at_].astype(f32), ins[5][at_], ins[8][at_], gwd_ref[0, k, h].astype(f32))
            for n, one in enumerate(new):
                outs[3 * n + 2][at_] = one


def update(ggu, gwd, weights, m, v):
    layers, rows, ff = weights[0].shape
    tiles = ff // TN
    gu = pl.BlockSpec((1, rows, TN), lambda n, j: (n, 0, j))
    wd = pl.BlockSpec((1, 32, weights[2].shape[2]), lambda n, j: (n, j, 0))
    specs = [gu, gu, wd] * 3
    arrays = (*weights, *m, *v)
    return pl.pallas_call(
        update_kernel,
        grid=(layers, tiles),
        in_specs=[
            pl.BlockSpec((1, 16, 1, 2, 16, U), lambda n, j: (n, 0, j, 0, 0, 0)),
            pl.BlockSpec((1, 2, 8, 16, U), lambda n, j: (n, j, 0, 0, 0)),
        ]
        + specs,
        out_specs=specs,
        out_shape=[jax.ShapeDtypeStruct(one.shape, one.dtype) for one in arrays],
        compiler_params=pltpu.CompilerParams(vmem_limit_bytes=48 * 2**20),
        name="update",
    )(ggu, gwd, *arrays)


def solution(mesh):
    def fetched(w, number):
        return lax.all_gather(w[number], "s", axis=0, tiled=True)

    def step(x, dy, *arrays):
        weights, m, v = (arrays[i : i + 3] for i in (0, 3, 6))
        w0 = [fetched(w, 0) for w in weights]
        w1 = [fetched(w, 1) for w in weights]
        s, t, p, h = forward(x[0], *w0)
        ggu, gwd = backward(x[0], h, dy[0], *w1, w0[2], s, t, p)
        return tuple(update(ggu, gwd, weights, m, v))

    states, cut = P(("rep", "r", "s"), None, None), P(None, "s", None)
    return jax.shard_map(
        step,
        mesh=mesh,
        in_specs=(states, states) + (cut,) * 9,
        out_specs=(P("rep", "s", None),) * 9,
        check_vma=False,
    )
```

```python
import functools

import jax
import jax.numpy as jnp
from jax import lax
from jax.experimental import pallas as pl
from jax.experimental.pallas import tpu as pltpu
from jax.sharding import PartitionSpec as P

MESH = pl.DeviceIdType.MESH
f32, bf16 = jnp.float32, jnp.bfloat16
TN = 256
MC = 512
U = 128
VMEM_LIMIT = 62 * 2**20


def dot(a, b):
    return lax.dot_general(a, b, (((1,), (0,)), ((), ())), preferred_element_type=f32)


def dot_nt(a, b):
    return lax.dot_general(a, b, (((1,), (1,)), ((), ())), preferred_element_type=f32)


def normed(h):
    wide = h.astype(f32)
    scale = lax.rsqrt(jnp.mean(wide**2, -1, keepdims=True) + 1e-6)
    return (wide * scale).astype(bf16)


def chunks(n, step):
    return [pl.ds(i, step) for i in range(0, n, step)]


def forward_kernel(tiles, x_ref, wg_in, wu_in, wd_in, s_ref, t_ref, p_ref, h_ref, wg_all, wu_all, wd_all,
                   a, acc, p_all, tg, tu, td, osem, orecv, lsem, asend, bsend, dsend, arecv, brecv, drecv):
    k = pl.program_id(0)
    tokens = x_ref.shape[0]
    r, s = lax.axis_index("r"), lax.axis_index("s")
    y, z, x, c = r // 4, r % 4, s // 2, s % 2
    items = 2 * tiles

    def remote(src, dst, ss, rs, dev):
        return pltpu.make_async_remote_copy(src_ref=src, dst_ref=dst, send_sem=ss, recv_sem=rs, device_id=dev, device_id_type=MESH)

    peer = (0, r, s + 1 - 2 * c)

    def own_copies():
        blocks = (
            (wg_in, wg_all.at[:, pl.ds(128 * s, 128), :]),
            (wu_in, wu_all.at[:, pl.ds(128 * s, 128), :]),
            (wd_in, wd_all.at[:, pl.ds(416 * s, 416), :]),
        )
        here = [pltpu.make_async_copy(src, dst, lsem.at[0, n]) for n, (src, dst) in enumerate(blocks)]
        there = [remote(src, dst, osem.at[n], orecv.at[n], peer) for n, (src, dst) in enumerate(blocks)]
        return here + there

    def parts(item, sx):
        layer, j = item // tiles, lax.rem(item, tiles)
        cols = pl.ds(pl.multiple_of(TN * j, TN), TN)
        owner = 2 * sx + c
        down = pl.ds(32 * j, 32), pl.ds(416 * owner + 32 * j, 32)
        return layer, (
            (wg_in, pl.ds(32 * y, 32), cols, wg_all, pl.ds(128 * owner + 32 * y, 32), "y"),
            (wu_in, pl.ds(32 * z, 32), cols, wu_all, pl.ds(128 * owner + 32 * z, 32), "z"),
            (wd_in, down[0], pl.ds(pl.multiple_of(128 * y, 128), 128), wd_all, down[1], "y"),
            (wd_in, down[0], pl.ds(pl.multiple_of(512 + 128 * z, 128), 128), wd_all, down[1], "z"),
        )

    def along(dim, d):
        if dim == "y":
            return (0, lax.rem(y + d, 4) * 4 + z, s)
        return (0, y * 4 + lax.rem(z + d, 4), s)

    def bytes_of(rows, sems, item, recv):
        some = wg_all.at[0, pl.ds(0, rows), pl.ds(0, 768)]
        if recv:
            pltpu.make_async_copy(some, some, sems.at[item]).wait()
        else:
            pltpu.make_async_copy(some, some, sems.at[0]).wait()

    @pl.when(k == 0)
    def _():
        for cp in own_copies():
            cp.start()

    @pl.when(k < items)
    def _():
        layer, some = parts(k, x)
        for d in (1, 2, 3):
            for src, rows, cols, dst, there, _dim in some:
                to = (0, r, 2 * lax.rem(x + d, 4) + c)
                remote(src.at[layer, rows, cols], dst.at[layer, there, cols], asend.at[0], arecv.at[k], to).start()

    @pl.when((k >= 2) & (k < items + 2))
    def _():
        item = k - 2
        bytes_of(96, arecv, item, True)
        for e in (1, 2, 3):
            layer, some = parts(item, lax.rem(x + e, 4))
            for _src, _rows, cols, dst, there, dim in some:
                ref = dst.at[layer, there, cols]
                for d in (1, 2, 3):
                    remote(ref, ref, bsend.at[0], brecv.at[item], along(dim, d)).start()

    @pl.when((k >= 4) & (k < items + 4))
    def _():
        item = k - 4
        bytes_of(288, brecv, item, True)
        layer, j = item // tiles, lax.rem(item, tiles)
        cols = pl.ds(pl.multiple_of(TN * j, TN), TN)
        for e in (1, 2, 3):
            owner = 2 * lax.rem(x + e, 4) + c
            for dst in (wg_all, wu_all):
                ref = dst.at[layer, pl.ds(128 * owner, 128), cols]
                remote(ref, ref, dsend.at[0], drecv.at[item], peer).start()
            ref = wd_all.at[layer, pl.ds(416 * owner + 32 * j, 32), :]
            remote(ref, ref, dsend.at[0], drecv.at[item], peer).start()

    @pl.when(k == 5)
    def _():
        for cp in own_copies():
            cp.wait()

    @pl.when(k == 0)
    def _():
        for rows in chunks(tokens, 256):
            a[rows, :] = normed(x_ref[rows, :])
            acc[rows, :] = jnp.zeros_like(acc[rows, :])

    def loads(tile):
        slot = lax.rem(tile, 2)
        cols = pl.ds(pl.multiple_of(TN * tile, TN), TN)
        return [
            pltpu.make_async_copy(wg_all.at[0, :, cols], tg.at[slot], lsem.at[1 + slot, 0]),
            pltpu.make_async_copy(wu_all.at[0, :, cols], tu.at[slot], lsem.at[1 + slot, 1]),
        ]

    def load_down(tile):
        slot = lax.rem(tile, 2)
        return pltpu.make_async_copy(wd_all.at[0, pl.ds(TN * tile, TN), :], td.at[slot], lsem.at[1 + slot, 2])

    @pl.when((k >= 5) & (k < items + 5))
    def _():
        bytes_of(384, drecv, k - 5, True)

    @pl.when((k >= 5) & (k < tiles + 5))
    def _():
        for cp in loads(k - 5):
            cp.start()

    @pl.when((k >= tiles + 5) & (k < items + 5))
    def _():
        load_down(k - tiles - 5).start()

    @pl.when((k >= 6) & (k < tiles + 6))
    def _():
        tile = k - 6
        slot = lax.rem(tile, 2)
        for cp in loads(tile):
            cp.wait()
        for rows in chunks(tokens, MC):
            g = dot(a[rows, :], tg[slot])
            u = dot(a[rows, :], tu[slot])
            sig = jax.nn.sigmoid(g)
            silu = g * sig
            s_ref[rows, :] = silu
            t_ref[rows, :] = u * (sig * (1 + g * (1 - sig)))
            p = (silu * u).astype(bf16)
            p_ref[rows, :] = p
            p_all[tile, rows, :] = p

    @pl.when((k >= tiles + 6) & (k < items + 6))
    def _():
        tile = k - tiles - 6
        load_down(tile).wait()
        for rows in chunks(tokens, MC):
            acc[rows, :] += dot(p_all[tile, rows, :], td[lax.rem(tile, 2)])

    @pl.when(k == items + 5)
    def _():
        for rows in chunks(tokens, 256):
            h_ref[rows, :] = (x_ref[rows, :].astype(f32) + acc[rows, :].astype(bf16).astype(f32)).astype(bf16)

        def sent(item, _):
            bytes_of(96, asend, item, False)
            bytes_of(288, bsend, item, False)
            bytes_of(384, dsend, item, False)
            return 0

        lax.fori_loop(0, items, sent, 0)


def forward(x, wg, wu, wd):
    tokens, d = x.shape
    ff = wg.shape[2]
    tiles = ff // TN
    one = pl.Buffered(1)
    anywhere = pl.BlockSpec(memory_space=pl.ANY)
    whole = pl.BlockSpec((tokens, d), lambda k: (0, 0), pipeline_mode=one)
    hid = pl.BlockSpec((tokens, TN), lambda k: (0, jnp.clip(k - 6, 0, tiles - 1)))
    ours = [pl.BlockSpec(w.shape, lambda k: (0, 0, 0), pipeline_mode=one) for w in (wg, wu, wd)]
    dma = pltpu.SemaphoreType.DMA
    return pl.pallas_call(
        functools.partial(forward_kernel, tiles),
        grid=(2 * tiles + 6,),
        in_specs=[whole, *ours],
        out_specs=[hid, hid, hid, whole, anywhere, anywhere, anywhere],
        out_shape=[jax.ShapeDtypeStruct((tokens, ff), f32)] * 2
        + [jax.ShapeDtypeStruct((tokens, ff), bf16), jax.ShapeDtypeStruct((tokens, d), bf16)]
        + [jax.ShapeDtypeStruct((2, d, ff), bf16)] * 2
        + [jax.ShapeDtypeStruct((2, ff, d), bf16)],
        scratch_shapes=[
            pltpu.VMEM((tokens, d), bf16),
            pltpu.VMEM((tokens, d), f32),
            pltpu.VMEM((tiles, tokens, TN), bf16),
            pltpu.VMEM((2, d, TN), bf16),
            pltpu.VMEM((2, d, TN), bf16),
            pltpu.VMEM((2, TN, d), bf16),
            dma((3,)),
            dma((3,)),
            dma((3, 3)),
            dma((1,)),
            dma((1,)),
            dma((1,)),
            dma((2 * tiles,)),
            dma((2 * tiles,)),
            dma((2 * tiles,)),
        ],
        compiler_params=pltpu.CompilerParams(vmem_limit_bytes=VMEM_LIMIT, has_side_effects=True),
        cost_estimate=pl.CostEstimate(flops=6 * tokens * d * ff, bytes_accessed=10 * tokens * ff, transcendentals=0),
        name="forward0",
    )(x, wg, wu, wd)


def backward_kernel(tiles, x_ref, h_ref, dy_ref, wg_ref, wu_ref, wd1_ref, wd0_ref, s_ref, t_ref, p_ref,
                    ggu_ref, gwd_ref,
                    a, at, dy, accg, accu, pbuf, dg, du, dgu, dwd, r0gu, r0wd, s1, r1, s2, r2, s3, r3, fin,
                    lsem, s0s, s0r, s1s, s1r, s2s, s2r, s3s, s3r, ags, agr, ago):
    i = pl.program_id(0)
    tokens = a.shape[0]
    r, s = lax.axis_index("r"), lax.axis_index("s")
    y, z, xx, c = r // 4, r % 4, s // 2, s % 2
    total = 2 * tiles
    where = {"x": xx, "y": y, "z": z}
    ORDER = ("yzx", "zxy", "xyz")

    def to(dim, d):
        if dim == "y":
            return (0, lax.rem(y + d, 4) * 4 + z, s)
        if dim == "z":
            return (0, y * 4 + lax.rem(z + d, 4), s)
        return (0, r, lax.rem(xx + d, 4) * 2 + c)

    def remote(src, dst, ss, rs, dev):
        return pltpu.make_async_remote_copy(src_ref=src, dst_ref=dst, send_sem=ss, recv_sem=rs, device_id=dev, device_id_type=MESH)

    def stage0(tile):
        slot = lax.rem(tile, 2)
        peer = (0, r, s + 1 - 2 * c)
        return [
            remote(dgu.at[:, :, 1 - c], r0gu.at[slot], s0s.at[0], s0r.at[slot, 0], peer),
            remote(dwd.at[1 - c], r0wd.at[slot], s0s.at[1], s0r.at[slot, 1], peer),
        ]

    def exchange(n, src, dst, ss, rs, tile):
        slot = lax.rem(tile, 2)
        copies = []
        for q in range(3):
            dim = ORDER[q][n]
            for d in (1, 2, 3):
                copies.append(
                    remote(src.at[q, lax.rem(where[dim] + d, 4)], dst.at[slot, q, d - 1], ss.at[q, d - 1], rs.at[slot, q, d - 1], to(dim, d))
                )
        return copies

    stages = [functools.partial(exchange, n, *refs) for n, refs in enumerate(((s1, r1, s1s, s1r), (s2, r2, s2s, s2r), (s3, r3, s3s, s3r)))]

    def added(n, src, dst, tile, q):
        slot = lax.rem(tile, 2)
        own = src[q, where[ORDER[q][n]]].astype(f32)
        return (own + dst[slot, q, 0].astype(f32) + dst[slot, q, 1].astype(f32) + dst[slot, q, 2].astype(f32)).astype(bf16)

    def spread(tile, d):
        layer, j = 1 - tile // tiles, lax.rem(tile, tiles)
        to_r = lax.rem(r + d, 16)
        row = 16 * j + r
        owner = row // 26
        gu = (fin.at[tile, pl.ds(0, 2)], ggu_ref.at[layer, r, j])
        wd = (fin.at[tile, 2], gwd_ref.at[layer, row - 26 * owner, 4 * c + xx])
        return gu, wd, (0, to_r, s), (0, to_r, owner), owner

    def own_spread(tile, act):
        gu, wd, _, to_wd, owner = spread(tile, 0)
        if act == "start":
            pltpu.make_async_copy(*gu, agr.at[0]).start()

        @pl.when(owner == s)
        def _():
            if act == "start":
                pltpu.make_async_copy(*wd, agr.at[1]).start()

        @pl.when(owner != s)
        def _():
            cp = remote(*wd, ago.at[0], agr.at[1], to_wd)
            cp.start() if act == "start" else cp.wait_send()

    @pl.when(i == 0)
    def _():
        cp = [pltpu.make_async_copy(h_ref, a, lsem.at[0]), pltpu.make_async_copy(dy_ref, dy, lsem.at[1])]
        cp[0].start()
        cp[1].start()
        cp[0].wait()
        for rows in chunks(tokens, 256):
            v = normed(a[rows, :])
            a[rows, :] = v
            at[:, rows] = v.T
            accg[rows, :] = jnp.zeros_like(accg[rows, :])
            accu[rows, :] = jnp.zeros_like(accu[rows, :])
        cp[1].wait()

    @pl.when(i < tiles)
    def _():
        for rows in chunks(tokens, MC):
            g = dot(a[rows, :], wg_ref[...])
            u = dot(a[rows, :], wu_ref[...])
            d = dot_nt(dy[rows, :], wd1_ref[...]).astype(bf16).astype(f32)
            sig = jax.nn.sigmoid(g)
            silu = g * sig
            pbuf[rows, :] = (silu * u).astype(bf16)
            du[rows, :] = (d * silu).astype(bf16)
            dg[rows, :] = (d * u * (sig * (1 + g * (1 - sig)))).astype(bf16)
        for rows in chunks(tokens, MC):
            accg[rows, :] += dot_nt(dg[rows, :], wg_ref[...])
            accu[rows, :] += dot_nt(du[rows, :], wu_ref[...])

    @pl.when((i >= tiles) & (i < total))
    def _():
        for rows in chunks(tokens, MC):
            d = dot_nt(dy[rows, :], wd0_ref[...]).astype(bf16).astype(f32)
            du[rows, :] = (d * s_ref[rows, :]).astype(bf16)
            dg[rows, :] = (d * t_ref[rows, :]).astype(bf16)
            pbuf[rows, :] = p_ref[rows, :]

    @pl.when((i >= 4) & (i < total + 4))
    def _():
        tile = i - 4
        for cp in stages[2](tile):
            cp.wait()
        for q in range(3):
            fin[tile, q] = added(2, s3, r3, tile, q)
        own_spread(tile, "start")

        def send(d, _):
            gu, wd, to_gu, to_wd, _o = spread(tile, d)
            remote(*gu, ags.at[0], agr.at[0], to_gu).start()
            remote(*wd, ags.at[1], agr.at[1], to_wd).start()
            return 0

        lax.fori_loop(1, 16, send, 0)

    @pl.when((i >= 3) & (i < total + 3))
    def _():
        tile = i - 3
        for cp in stages[1](tile):
            cp.wait()
        for q in range(3):
            s3[q] = added(1, s2, r2, tile, q)
        for cp in stages[2](tile):
            cp.start()

    @pl.when((i >= 2) & (i < total + 2))
    def _():
        tile = i - 2
        for cp in stages[0](tile):
            cp.wait()
        for q in range(3):
            s2[q] = added(0, s1, r1, tile, q)
        for cp in stages[1](tile):
            cp.start()

    @pl.when((i >= 1) & (i < total + 1))
    def _():
        tile = i - 1
        slot = lax.rem(tile, 2)
        for cp in stage0(tile):
            cp.wait()
        for xi in range(4):
            for k in range(8):
                for h in range(2):
                    rows, cols = pl.ds(16 * k, 16), pl.ds(U * h, U)
                    yi, zi = k // 2, 2 * (k % 2) + h
                    for q, at_ in ((0, (yi, zi, xi)), (1, (zi, xi, yi))):
                        v = dgu[q, xi, c, rows, cols].astype(f32) + r0gu[slot, q, xi, rows, cols].astype(f32)
                        s1[(q, *at_)] = v.astype(bf16)
                    unit = 2 * k + h
                    rows, cols = pl.ds(16 * unit, 16), pl.ds(U * xi, U)
                    v = dwd[c, rows, cols].astype(f32) + r0wd[slot, rows, cols].astype(f32)
                    s1[2, xi, unit // 4, unit % 4] = v.astype(bf16)
        for cp in stages[0](tile):
            cp.start()

    @pl.when(i < total)
    def _():
        for q, one in ((0, dg), (1, du)):
            g = dot(at[...], one[...]).astype(bf16)
            dgu[q] = g.reshape(dgu.shape[1:])
        g = dot(pbuf[...].T, dy[...]).astype(bf16)
        dwd[0] = g[:, :512]
        dwd[1] = g[:, 512:]
        for cp in stage0(i):
            cp.start()

    @pl.when(i == tiles - 1)
    def _():
        cp = pltpu.make_async_copy(h_ref, a, lsem.at[0])
        cp.start()
        cp.wait()
        for rows in chunks(tokens, 256):
            da = (accg[rows, :].astype(bf16).astype(f32) + accu[rows, :].astype(bf16).astype(f32)).astype(bf16).astype(f32)
            wide = a[rows, :].astype(f32)
            scale = lax.rsqrt(jnp.mean(wide**2, -1, keepdims=True) + 1e-6)
            along = jnp.sum(da * wide, -1, keepdims=True)
            by_h = da * scale - wide * (along * (scale * scale * scale) * (1.0 / wide.shape[-1]))
            dy[rows, :] = (dy[rows, :].astype(f32) + by_h.astype(bf16).astype(f32)).astype(bf16)
        cp = pltpu.make_async_copy(x_ref, a, lsem.at[0])
        cp.start()
        cp.wait()
        for rows in chunks(tokens, 256):
            at[:, rows] = normed(a[rows, :]).T

    @pl.when(i == total + 3)
    def _():
        remote(ggu_ref.at[:, pl.ds(0, 15)], ggu_ref.at[:, pl.ds(0, 15)], ags.at[0], agr.at[0], to("y", 1)).wait_send()
        half = ggu_ref.at[0, pl.ds(0, 15)]
        remote(half, half, ags.at[1], agr.at[1], to("y", 1)).wait_send()

        def done(tile, _):
            own_spread(tile, "wait")
            return 0

        lax.fori_loop(0, total, done, 0)
        pltpu.make_async_copy(ggu_ref, ggu_ref, agr.at[0]).wait()
        pltpu.make_async_copy(gwd_ref, gwd_ref, agr.at[1]).wait()


def backward(x, h, dy, wg, wu, wd, s, t, p):
    tokens, d = x.shape
    ff = wg.shape[2]
    tiles = ff // TN
    last = tiles - 1
    anywhere = pl.BlockSpec(memory_space=pl.ANY)
    cols = pl.BlockSpec((None, d, TN), lambda i: (1, 0, jnp.minimum(i, last)))
    clamp = lambda i: jnp.clip(i - tiles, 0, last)
    hid = pl.BlockSpec((tokens, TN), lambda i: (0, clamp(i)))
    dma = pltpu.SemaphoreType.DMA
    unit = (16, U)
    return pl.pallas_call(
        functools.partial(backward_kernel, tiles),
        grid=(2 * tiles + 4,),
        in_specs=[anywhere] * 3
        + [cols, cols, pl.BlockSpec((None, TN, d), lambda i: (1, jnp.minimum(i, last), 0)), pl.BlockSpec((None, TN, d), lambda i: (0, clamp(i), 0))]
        + [hid] * 3,
        out_specs=[anywhere] * 2,
        out_shape=[jax.ShapeDtypeStruct((2, 16, tiles, 2, *unit), bf16), jax.ShapeDtypeStruct((2, 26, 8, *unit), bf16)],
        scratch_shapes=[
            pltpu.VMEM((tokens, d), bf16),
            pltpu.VMEM((d, tokens), bf16),
            pltpu.VMEM((tokens, d), bf16),
            pltpu.VMEM((tokens, d), f32),
            pltpu.VMEM((tokens, d), f32),
            pltpu.VMEM((tokens, TN), bf16),
            pltpu.VMEM((tokens, TN), bf16),
            pltpu.VMEM((tokens, TN), bf16),
            pltpu.VMEM((2, 4, 2, 128, TN), bf16),
            pltpu.VMEM((2, TN, 512), bf16),
            pltpu.VMEM((2, 2, 4, 128, TN), bf16),
            pltpu.VMEM((2, TN, 512), bf16),
            pltpu.VMEM((3, 4, 4, 4, *unit), bf16),
            pltpu.VMEM((2, 3, 3, 4, 4, *unit), bf16),
            pltpu.VMEM((3, 4, 4, *unit), bf16),
            pltpu.VMEM((2, 3, 3, 4, *unit), bf16),
            pltpu.VMEM((3, 4, *unit), bf16),
            pltpu.VMEM((2, 3, 3, *unit), bf16),
            pltpu.VMEM((2 * tiles, 3, *unit), bf16),
            dma((2,)),
            dma((2,)),
            dma((2, 2)),
        ]
        + [dma((3, 3)), dma((2, 3, 3))] * 3
        + [dma((2,)), dma((2,)), dma((1,))],
        compiler_params=pltpu.CompilerParams(vmem_limit_bytes=VMEM_LIMIT, has_side_effects=True),
        cost_estimate=pl.CostEstimate(flops=24 * tokens * d * ff, bytes_accessed=10 * tokens * ff, transcendentals=0),
        name="backward",
    )(x, h, dy, wg, wu, wd, wd, s, t, p)


def adamw(w, m, v, g):
    m = 0.9 * m + 0.1 * g
    v = 0.95 * v + 0.05 * g * g
    step = m * lax.rsqrt(v + 1e-8) + 0.1 * w
    return (w - 0.02 * step).astype(bf16), m, v


def update_kernel(ggu_ref, gwd_ref, *refs):
    ins, outs = refs[:9], refs[9:]
    for q in range(2):
        for k in range(8):
            for h in range(2):
                at_ = (0, pl.ds(16 * k, 16), pl.ds(U * h, U))
                new = adamw(ins[q][at_].astype(f32), ins[3 + q][at_], ins[6 + q][at_], ggu_ref[0, 2 * k + h, 0, q].astype(f32))
                for n, one in enumerate(new):
                    outs[3 * n + q][at_] = one
    for k in range(2):
        for h in range(8):
            at_ = (0, pl.ds(16 * k, 16), pl.ds(U * h, U))
            new = adamw(ins[2][at_].astype(f32), ins[5][at_], ins[8][at_], gwd_ref[0, k, h].astype(f32))
            for n, one in enumerate(new):
                outs[3 * n + 2][at_] = one


def update(ggu, gwd, weights, m, v):
    layers, rows, ff = weights[0].shape
    tiles = ff // TN
    gu = pl.BlockSpec((1, rows, TN), lambda n, j: (n, 0, j))
    wd = pl.BlockSpec((1, 32, weights[2].shape[2]), lambda n, j: (n, j, 0))
    specs = [gu, gu, wd] * 3
    arrays = (*weights, *m, *v)
    return pl.pallas_call(
        update_kernel,
        grid=(layers, tiles),
        in_specs=[
            pl.BlockSpec((1, 16, 1, 2, 16, U), lambda n, j: (n, 0, j, 0, 0, 0)),
            pl.BlockSpec((1, 2, 8, 16, U), lambda n, j: (n, j, 0, 0, 0)),
        ]
        + specs,
        out_specs=specs,
        out_shape=[jax.ShapeDtypeStruct(one.shape, one.dtype) for one in arrays],
        compiler_params=pltpu.CompilerParams(vmem_limit_bytes=48 * 2**20),
        name="update",
    )(ggu, gwd, *arrays)


def solution(mesh):
    def step(x, dy, *arrays):
        weights, m, v = (arrays[i : i + 3] for i in (0, 3, 6))
        s, t, p, h, *whole = forward(x[0], *weights)
        ggu, gwd = backward(x[0], h, dy[0], *whole, s, t, p)
        return tuple(update(ggu, gwd, weights, m, v))

    states, cut = P(("rep", "r", "s"), None, None), P(None, "s", None)
    return jax.shard_map(
        step,
        mesh=mesh,
        in_specs=(states, states) + (cut,) * 9,
        out_specs=(P("rep", "s", None),) * 9,
        check_vma=False,
    )
```

```python
import functools

import jax
import jax.numpy as jnp
from jax import lax
from jax.experimental import pallas as pl
from jax.experimental.pallas import tpu as pltpu
from jax.sharding import PartitionSpec as P

MESH = pl.DeviceIdType.MESH
f32, bf16 = jnp.float32, jnp.bfloat16
TN = 256
MC = 512
U = 128
VMEM_LIMIT = 67043328


def dot(a, b):
    return lax.dot_general(a, b, (((1,), (0,)), ((), ())), preferred_element_type=f32)


def dot_nt(a, b):
    return lax.dot_general(a, b, (((1,), (1,)), ((), ())), preferred_element_type=f32)


def normed(h):
    wide = h.astype(f32)
    scale = lax.rsqrt(jnp.mean(wide**2, -1, keepdims=True) + 1e-6)
    return (wide * scale).astype(bf16)


def chunks(n, step):
    return [pl.ds(i, step) for i in range(0, n, step)]


class Place:
    def __init__(self):
        self.r, self.s = lax.axis_index("r"), lax.axis_index("s")
        self.y, self.z, self.x, self.c = self.r // 4, self.r % 4, self.s // 2, self.s % 2
        self.peer = (0, self.r, self.s + 1 - 2 * self.c)

    def along(self, dim, d):
        if dim == "y":
            return (0, lax.rem(self.y + d, 4) * 4 + self.z, self.s)
        if dim == "z":
            return (0, self.y * 4 + lax.rem(self.z + d, 4), self.s)
        return (0, self.r, lax.rem(self.x + d, 4) * 2 + self.c)


def remote(src, dst, ss, rs, dev):
    return pltpu.make_async_remote_copy(src_ref=src, dst_ref=dst, send_sem=ss, recv_sem=rs, device_id=dev, device_id_type=MESH)


class Fetch:
    A, B, D = 288, 864, 1152

    def __init__(self, place, own, whole, some, sends, recvs):
        self.p, self.own, self.whole, self.some, self.sends, self.recvs = place, own, whole, some, sends, recvs

    def quarters(self, refs, owner):
        p, (wg, wu, wd) = self.p, refs
        base, low = (0, 0) if owner is None else (128 * owner, 32 * owner)
        rows = pl.ds(low, 32)
        return (
            (wg.at[pl.ds(base + 32 * p.y, 32), :], "y"),
            (wu.at[pl.ds(base + 32 * p.z, 32), :], "z"),
            (wd.at[rows, pl.ds(pl.multiple_of(128 * p.y, 128), 128)], "y"),
            (wd.at[rows, pl.ds(pl.multiple_of(512 + 128 * p.z, 128), 128)], "z"),
        )

    def wait(self, rows, sem):
        some = self.some.at[pl.ds(0, 1), pl.ds(0, rows)] if rows <= 1024 else self.some.at[pl.ds(0, 2), pl.ds(0, rows // 2)]
        pltpu.make_async_copy(some, some, sem).wait()

    def a(self, tile, n):
        src, dst = self.quarters(self.own(tile), None), self.quarters(self.whole(tile), self.p.s)
        for d in (1, 2, 3):
            for (one, _), (other, _) in zip(src, dst, strict=True):
                remote(one, other, self.sends.at[0], self.recvs[0].at[n], self.p.along("x", d)).start()

    def b(self, tile, n):
        self.wait(self.A, self.recvs[0].at[n])
        for e in (1, 2, 3):
            for ref, dim in self.quarters(self.whole(tile), 2 * lax.rem(self.p.x + e, 4) + self.p.c):
                for d in (1, 2, 3):
                    remote(ref, ref, self.sends.at[1], self.recvs[1].at[n], self.p.along(dim, d)).start()

    def d(self, tile, n):
        self.wait(self.B, self.recvs[1].at[n])
        wg, wu, wd = self.whole(tile)
        for e in (1, 2, 3):
            owner = 2 * lax.rem(self.p.x + e, 4) + self.p.c
            for ref in (wg.at[pl.ds(128 * owner, 128), :], wu.at[pl.ds(128 * owner, 128), :], wd.at[pl.ds(32 * owner, 32), :]):
                remote(ref, ref, self.sends.at[2], self.recvs[2].at[n], self.p.peer).start()

    def here(self, n):
        self.wait(self.D, self.recvs[2].at[n])

    def sent(self, count):
        def one(_n, _):
            for k, rows in enumerate((self.A, self.B, self.D)):
                self.wait(rows, self.sends.at[k])
            return 0

        lax.fori_loop(0, count, one, 0)


def forward_kernel(tiles, early, x_ref, wg_in, wu_in, wd_in, s_ref, t_ref, p_ref, h_ref, wg_all, wu_all, wd_all,
                   a, acc, wgp, wup, tg, tu, td, osem, orecv, lsem, sends, arecv, brecv, drecv):
    k = pl.program_id(0)
    tokens = x_ref.shape[0]
    place = Place()
    fetch = [
        Fetch(
            place,
            lambda j, n=n: (wgp.at[n, j], wup.at[n, j], wd_in.at[n, j]),
            lambda j, n=n: (wg_all.at[n, j], wu_all.at[n, j], wd_all.at[n, j]),
            wg_all.at[0],
            sends,
            (arecv, brecv, drecv),
        )
        for n in range(2)
    ]

    def own_copies(n):
        blocks = (
            (wgp.at[n], wg_all.at[n, :, pl.ds(128 * place.s, 128), :]),
            (wup.at[n], wu_all.at[n, :, pl.ds(128 * place.s, 128), :]),
            (wd_in.at[n], wd_all.at[n, :, pl.ds(32 * place.s, 32), :]),
        )
        here = [pltpu.make_async_copy(src, dst, lsem.at[n, m]) for m, (src, dst) in enumerate(blocks)]
        there = [remote(src, dst, osem.at[n, m], orecv.at[n, m], place.peer) for m, (src, dst) in enumerate(blocks)]
        return here + there

    def permute(n):
        def rows_of(i, _):
            rows = pl.ds(pl.multiple_of(16 * i, 16), 16)
            for src, dst in ((wg_in, wgp), (wu_in, wup)):
                v = src[n, rows, :]
                for j in range(tiles):
                    for h in range(2):
                        parts = [v[:, 416 * o + 32 * j : 416 * o + 32 * j + 32] for o in range(4 * h, 4 * h + 4)]
                        dst[n, j, rows, U * h : U * h + U] = jnp.concatenate(parts, axis=1)
            return 0

        lax.fori_loop(0, 8, rows_of, 0)

    for n in range(2):

        @pl.when(k == n)
        def _(n=n):
            permute(n)
            for cp in own_copies(n):
                cp.start()

    @pl.when(k < tiles)
    def _():
        fetch[0].a(k, k)

    m = k // 2 - 2
    even = lax.rem(k, 2) == 0

    @pl.when(even & (m >= 0) & (m < early))
    def _():
        fetch[1].a(m, tiles + m)

    @pl.when((k >= 2) & (k < tiles + 2))
    def _():
        fetch[0].b(k - 2, k - 2)

    @pl.when(even & (m >= 1) & (m < early + 1))
    def _():
        fetch[1].b(m - 1, tiles + m - 1)

    @pl.when((k >= 4) & (k < tiles + 4))
    def _():
        fetch[0].d(k - 4, k - 4)

    @pl.when(even & (m >= 2) & (m < early + 2))
    def _():
        fetch[1].d(m - 2, tiles + m - 2)

    @pl.when(k == 0)
    def _():
        for rows in chunks(tokens, 256):
            a[rows, :] = normed(x_ref[rows, :])
            acc[rows, :] = jnp.zeros_like(acc[rows, :])

    for n in range(2):

        @pl.when(k == 4 + n)
        def _(n=n):
            for cp in own_copies(n):
                cp.wait()

    def loads(tile):
        slot = lax.rem(tile, 2)
        pairs = ((wg_all.at[0, tile], tg), (wu_all.at[0, tile], tu), (wd_all.at[0, tile], td))
        return [pltpu.make_async_copy(src, dst.at[slot], lsem.at[2 + slot, q]) for q, (src, dst) in enumerate(pairs)]

    @pl.when((k >= 5) & (k < tiles + 5))
    def _():
        fetch[0].here(k - 5)
        for cp in loads(k - 5):
            cp.start()

    @pl.when(k >= 6)
    def _():
        tile = k - 6
        slot = lax.rem(tile, 2)
        for cp in loads(tile):
            cp.wait()
        for rows in chunks(tokens, MC):
            g = dot(a[rows, :], tg[slot])
            u = dot(a[rows, :], tu[slot])
            sig = jax.nn.sigmoid(g)
            silu = g * sig
            s_ref[rows, :] = silu
            t_ref[rows, :] = u * (sig * (1 + g * (1 - sig)))
            p_ref[rows, :] = (silu * u).astype(bf16)
        for rows in chunks(tokens, MC):
            acc[rows, :] += dot(p_ref[rows, :], td[slot])

    @pl.when(k == tiles + 5)
    def _():
        for rows in chunks(tokens, 256):
            h_ref[rows, :] = (x_ref[rows, :].astype(f32) + acc[rows, :].astype(bf16).astype(f32)).astype(bf16)
        for n in range(early):
            fetch[1].here(tiles + n)
        fetch[0].sent(tiles + early)


def forward(x, wg, wu, wd, early):
    tokens, d = x.shape
    ff = wg.shape[2]
    tiles = ff // TN
    one = pl.Buffered(1)
    anywhere = pl.BlockSpec(memory_space=pl.ANY)
    whole = pl.BlockSpec((tokens, d), lambda k: (0, 0), pipeline_mode=one)
    hid = pl.BlockSpec((tokens, TN), lambda k: (0, jnp.clip(k - 6, 0, tiles - 1)))
    wd = wd.reshape(2, tiles, 32, d)
    ours = [pl.BlockSpec(w.shape, lambda k, n=w.ndim: (0,) * n, pipeline_mode=one) for w in (wg, wu, wd)]
    dma = pltpu.SemaphoreType.DMA
    return pl.pallas_call(
        functools.partial(forward_kernel, tiles, early),
        grid=(tiles + 6,),
        in_specs=[whole, *ours],
        out_specs=[hid, hid, hid, whole, anywhere, anywhere, anywhere],
        out_shape=[jax.ShapeDtypeStruct((tokens, ff), f32)] * 2
        + [jax.ShapeDtypeStruct((tokens, ff), bf16), jax.ShapeDtypeStruct((tokens, d), bf16)]
        + [jax.ShapeDtypeStruct((2, tiles, d, TN), bf16)] * 2
        + [jax.ShapeDtypeStruct((2, tiles, TN, d), bf16)],
        scratch_shapes=[
            pltpu.VMEM((tokens, d), bf16),
            pltpu.VMEM((tokens, d), f32),
            pltpu.VMEM((2, tiles, 128, TN), bf16),
            pltpu.VMEM((2, tiles, 128, TN), bf16),
            pltpu.VMEM((2, d, TN), bf16),
            pltpu.VMEM((2, d, TN), bf16),
            pltpu.VMEM((2, TN, d), bf16),
            dma((2, 3)),
            dma((2, 3)),
            dma((4, 3)),
            dma((3,)),
            dma((tiles + early,)),
            dma((tiles + early,)),
            dma((tiles + early,)),
        ],
        compiler_params=pltpu.CompilerParams(vmem_limit_bytes=VMEM_LIMIT, has_side_effects=True),
        cost_estimate=pl.CostEstimate(flops=6 * tokens * d * ff, bytes_accessed=10 * tokens * ff, transcendentals=0),
        name="forward0",
    )(x, wg, wu, wd)


def backward_kernel(tiles, early, x_ref, h_ref, dy_ref, wg_ref, wu_ref, wd_ref, wd0_ref, s_ref, t_ref, p_ref,
                    sums_ref, wg_more, wu_more, wd_more,
                    a, at, dy, accg, accu, pbuf, dg, du, tg, tu, td, dgu, dwd, r0gu, r0wd, s1, r1, s2, r2, s3, r3, fin,
                    lsem, tsem, s0s, s0r, s1s, s1r, s2s, s2r, s3s, s3r, ags, agr, sends, arecv, brecv, drecv):
    i = pl.program_id(0)
    tokens = a.shape[0]
    place = Place()
    r, c = place.r, place.c
    total = 2 * tiles
    where = {"x": place.x, "y": place.y, "z": place.z}
    ORDER = ("yzx", "zxy", "xyz")

    def stage0(tile):
        slot = lax.rem(tile, 2)
        return [
            remote(dgu.at[slot, :, :, 1 - c], r0gu.at[slot], s0s.at[slot, 0], s0r.at[slot, 0], place.peer),
            remote(dwd.at[slot, :, 1 - c], r0wd.at[slot], s0s.at[slot, 1], s0r.at[slot, 1], place.peer),
        ]

    STAGES = ((s1, r1, s1s, s1r, 2, 4), (s2, r2, s2s, s2r, 1, 2), (s3, r3, s3s, s3r, 1, 2))

    def exchange(n, tile):
        src, dst, ss, rs, held, slots = STAGES[n]
        own, slot = lax.rem(tile, held), lax.rem(tile, slots)
        for q in range(3):
            dim = ORDER[q][n]
            for d in (1, 2, 3):
                part = src.at[own, q, lax.rem(where[dim] + d, 4)]
                remote(part, dst.at[slot, q, d - 1], ss.at[own], rs.at[slot], place.along(dim, d)).start()

    def arrived(n, tile):
        src, dst, ss, rs, held, slots = STAGES[n]
        own, slot = lax.rem(tile, held), lax.rem(tile, slots)
        sent = src.at[own, :, pl.ds(0, 3)]
        pltpu.make_async_copy(sent, sent, ss.at[own]).wait()
        pltpu.make_async_copy(dst.at[slot], dst.at[slot], rs.at[slot]).wait()

    def added(n, tile, q):
        src, dst, _ss, _rs, held, slots = STAGES[n]
        slot = lax.rem(tile, slots)
        own = src[lax.rem(tile, held), q, where[ORDER[q][n]]].astype(f32)
        return (own + dst[slot, q, 0].astype(f32) + dst[slot, q, 1].astype(f32) + dst[slot, q, 2].astype(f32)).astype(bf16)

    def spread(tile):
        src, dst = fin.at[tile], sums_ref.at[1 - tile // tiles, r, lax.rem(tile, tiles)]
        pltpu.make_async_copy(src, dst, agr.at[0]).start()

        def one(d, _):
            remote(src, dst, ags.at[0], agr.at[0], (0, lax.rem(r + d, 16), place.s)).start()
            return 0

        lax.fori_loop(1, 16, one, 0)

    fetch = Fetch(
        place,
        lambda j: (wg_ref.at[1, j, pl.ds(128 * place.s, 128), :], wu_ref.at[1, j, pl.ds(128 * place.s, 128), :], wd_ref.at[1, j, pl.ds(32 * place.s, 32), :]),
        lambda j: (wg_more.at[j - early], wu_more.at[j - early], wd_more.at[j - early]),
        wg_more,
        sends,
        (arecv, brecv, drecv),
    )

    def load(tile, act):
        slot = lax.rem(tile, 2)
        arrays = ((wg_ref, wg_more, tg, 256), (wu_ref, wu_more, tu, 256), (wd_ref, wd_more, td, 64))

        @pl.when(tile < early)
        def _():
            for q, (first, _more, dst, _n) in enumerate(arrays):
                act(pltpu.make_async_copy(first.at[1, tile], dst.at[slot], tsem.at[slot, q]))

        @pl.when(tile >= early)
        def _():
            for q, (first, more, dst, n) in enumerate(arrays):
                for e in range(4):
                    rows = pl.ds(n * lax.rem(place.x + e, 4), n)
                    src = first.at[1, tile, rows, :] if e == 0 else more.at[tile - early, rows, :]
                    cp = pltpu.make_async_copy(src, dst.at[slot, rows, :], tsem.at[slot, q])
                    act(cp)

    @pl.when(i == 0)
    def _():
        cp = [pltpu.make_async_copy(h_ref, a, lsem.at[0]), pltpu.make_async_copy(dy_ref, dy, lsem.at[1])]
        cp[0].start()
        cp[1].start()
        load(i, lambda cp: cp.start())
        cp[0].wait()
        for rows in chunks(tokens, 256):
            v = normed(a[rows, :])
            a[rows, :] = v
            at[:, rows] = v.T
            accg[rows, :] = jnp.zeros_like(accg[rows, :])
            accu[rows, :] = jnp.zeros_like(accu[rows, :])
        cp[1].wait()

    @pl.when((i >= early - 1) & (i < tiles - 1))
    def _():
        fetch.here(i + 1 - early)

    @pl.when(i < tiles - 1)
    def _():
        load(i + 1, lambda cp: cp.start())

    def by_weights(p):
        slot = lax.rem(i, 2)
        for q, one in ((0, dg), (1, du)):
            dgu[slot, q] = dot(at[...], one[...]).astype(bf16).reshape(dgu.shape[2:])
        dwd[slot] = dot(p[...].T, dy[...]).astype(bf16).reshape(dwd.shape[1:])

    @pl.when(i < tiles)
    def _():
        slot = lax.rem(i, 2)
        load(i, lambda cp: cp.wait())
        for rows in chunks(tokens, MC):
            g = dot(a[rows, :], tg[slot])
            u = dot(a[rows, :], tu[slot])
            d = dot_nt(dy[rows, :], td[slot]).astype(bf16).astype(f32)
            sig = jax.nn.sigmoid(g)
            silu = g * sig
            pbuf[rows, :] = (silu * u).astype(bf16)
            du[rows, :] = (d * silu).astype(bf16)
            dg[rows, :] = (d * u * (sig * (1 + g * (1 - sig)))).astype(bf16)
        for rows in chunks(tokens, MC):
            accg[rows, :] += dot_nt(dg[rows, :], tg[slot])
            accu[rows, :] += dot_nt(du[rows, :], tu[slot])
        by_weights(pbuf)

    @pl.when((i >= tiles) & (i < total))
    def _():
        for rows in chunks(tokens, MC):
            d = dot_nt(dy[rows, :], wd0_ref[...]).astype(bf16).astype(f32)
            du[rows, :] = (d * s_ref[rows, :]).astype(bf16)
            dg[rows, :] = (d * t_ref[rows, :]).astype(bf16)
        by_weights(p_ref)

    @pl.when(i == tiles - 1)
    def _():
        pltpu.make_async_copy(h_ref, a, lsem.at[0]).start()

    @pl.when((i >= 5) & (i < total + 5))
    def _():
        tile = i - 5
        arrived(2, tile)
        for q in range(3):
            fin[tile, q] = added(2, tile, q)

    @pl.when((i >= 4) & (i < total + 4))
    def _():
        tile = i - 4
        arrived(1, tile)
        for q in range(3):
            s3[0, q] = added(1, tile, q)
        exchange(2, tile)

    @pl.when((i >= 3) & (i < total + 3))
    def _():
        tile = i - 3
        arrived(0, tile)
        for q in range(3):
            s2[0, q] = added(0, tile, q)
        exchange(1, tile)

    @pl.when((i >= 1) & (i < total + 1))
    def _():
        tile = i - 1
        slot = lax.rem(tile, 2)
        for cp in stage0(tile):
            cp.wait()
        for xi in range(4):
            for k in range(8):
                for h in range(2):
                    rows, cols = pl.ds(16 * k, 16), pl.ds(U * h, U)
                    yi, zi = k // 2, 2 * (k % 2) + h
                    for q, at_ in ((0, (yi, zi, xi)), (1, (zi, xi, yi))):
                        v = dgu[slot, q, xi, c, rows, cols].astype(f32) + r0gu[slot, q, xi, rows, cols].astype(f32)
                        s1[(slot, q, *at_)] = v.astype(bf16)
                    rows, cols = pl.ds(16 * (yi // 2), 16), pl.ds(U * (4 * (yi % 2) + zi), U)
                    v = dwd[slot, xi, c, rows, cols].astype(f32) + r0wd[slot, xi, rows, cols].astype(f32)
                    s1[slot, 2, xi, yi, zi] = v.astype(bf16)
        exchange(0, tile)

    @pl.when(i < total)
    def _():
        for cp in stage0(i):
            cp.start()

    for stage, lag in ((fetch.d, 3), (fetch.b, 4), (fetch.a, 5)):

        @pl.when((i + lag >= early) & (i + lag < tiles))
        def _(stage=stage, lag=lag):
            stage(i + lag, i + lag - early)

    @pl.when((i >= 5) & (i < total + 5))
    def _():
        spread(i - 5)

    @pl.when(i == tiles - 1)
    def _():
        pltpu.make_async_copy(h_ref, a, lsem.at[0]).wait()
        parts = chunks(tokens, 256)
        for n, rows in enumerate(parts):
            da = (accg[rows, :].astype(bf16).astype(f32) + accu[rows, :].astype(bf16).astype(f32)).astype(bf16).astype(f32)
            wide = a[rows, :].astype(f32)
            scale = lax.rsqrt(jnp.mean(wide**2, -1, keepdims=True) + 1e-6)
            along = jnp.sum(da * wide, -1, keepdims=True)
            by_h = da * scale - wide * (along * (scale * scale * scale) * (1.0 / wide.shape[-1]))
            dy[rows, :] = (dy[rows, :].astype(f32) + by_h.astype(bf16).astype(f32)).astype(bf16)
            pltpu.make_async_copy(x_ref.at[rows, :], a.at[rows, :], lsem.at[n]).start()
        for n, rows in enumerate(parts):
            pltpu.make_async_copy(x_ref.at[rows, :], a.at[rows, :], lsem.at[n]).wait()
            at[:, rows] = normed(a[rows, :]).T

    @pl.when(i == total + 4)
    def _():
        fetch.sent(tiles - early)
        some = sums_ref.at[:, pl.ds(0, 15)]
        pltpu.make_async_copy(some, some, ags.at[0]).wait()
        pltpu.make_async_copy(sums_ref, sums_ref, agr.at[0]).wait()


def backward(x, h, dy, wg, wu, wd, s, t, p, early):
    tokens, d = x.shape
    ff = s.shape[1]
    tiles = ff // TN
    last = tiles - 1
    anywhere = pl.BlockSpec(memory_space=pl.ANY)
    clamp = lambda i: jnp.clip(i - tiles, 0, last)
    hid = pl.BlockSpec((tokens, TN), lambda i: (0, clamp(i)))
    dma = pltpu.SemaphoreType.DMA
    unit = (16, U)
    return pl.pallas_call(
        functools.partial(backward_kernel, tiles, early),
        grid=(2 * tiles + 5,),
        in_specs=[anywhere] * 6 + [pl.BlockSpec((None, None, TN, d), lambda i: (0, clamp(i), 0, 0))] + [hid] * 3,
        out_specs=[anywhere] * 4,
        out_shape=[
            jax.ShapeDtypeStruct((2, 16, tiles, 3, *unit), bf16),
            jax.ShapeDtypeStruct((tiles - early, d, TN), bf16),
            jax.ShapeDtypeStruct((tiles - early, d, TN), bf16),
            jax.ShapeDtypeStruct((tiles - early, TN, d), bf16),
        ],
        scratch_shapes=[
            pltpu.VMEM((tokens, d), bf16),
            pltpu.VMEM((d, tokens), bf16),
            pltpu.VMEM((tokens, d), bf16),
            pltpu.VMEM((tokens, d), f32),
            pltpu.VMEM((tokens, d), f32),
            pltpu.VMEM((tokens, TN), bf16),
            pltpu.VMEM((tokens, TN), bf16),
            pltpu.VMEM((tokens, TN), bf16),
            pltpu.VMEM((2, d, TN), bf16),
            pltpu.VMEM((2, d, TN), bf16),
            pltpu.VMEM((2, TN, d), bf16),
            pltpu.VMEM((2, 2, 4, 2, 128, TN), bf16),
            pltpu.VMEM((2, 4, 2, 32, d), bf16),
            pltpu.VMEM((2, 2, 4, 128, TN), bf16),
            pltpu.VMEM((2, 4, 32, d), bf16),
            pltpu.VMEM((2, 3, 4, 4, 4, *unit), bf16),
            pltpu.VMEM((4, 3, 3, 4, 4, *unit), bf16),
            pltpu.VMEM((1, 3, 4, 4, *unit), bf16),
            pltpu.VMEM((2, 3, 3, 4, *unit), bf16),
            pltpu.VMEM((1, 3, 4, *unit), bf16),
            pltpu.VMEM((2, 3, 3, *unit), bf16),
            pltpu.VMEM((2 * tiles, 3, *unit), bf16),
            dma((8,)),
            dma((2, 3)),
            dma((2, 2)),
            dma((2, 2)),
            dma((2,)),
            dma((4,)),
            dma((1,)),
            dma((2,)),
            dma((1,)),
            dma((2,)),
            dma((1,)),
            dma((1,)),
            dma((3,)),
            dma((tiles - early,)),
            dma((tiles - early,)),
            dma((tiles - early,)),
        ],
        compiler_params=pltpu.CompilerParams(vmem_limit_bytes=VMEM_LIMIT, has_side_effects=True),
        cost_estimate=pl.CostEstimate(flops=24 * tokens * d * ff, bytes_accessed=10 * tokens * ff, transcendentals=0),
        name="backward",
    )(x, h, dy, wg, wu, wd, wd, s, t, p)[0]


def adamw(w, m, v, g):
    m = 0.9 * m + 0.1 * g
    v = 0.95 * v + 0.05 * g * g
    step = m * lax.rsqrt(v + 1e-8) + 0.1 * w
    return (w - 0.02 * step).astype(bf16), m, v


def update_kernel(tiles, sgu_ref, sd_ref, *refs):
    ins, outs = refs[:9], refs[9:]
    i = pl.program_id(0)

    def one(q, at_, g):
        new = adamw(ins[q][at_].astype(f32), ins[3 + q][at_], ins[6 + q][at_], g.astype(f32))
        for n, value in enumerate(new):
            outs[3 * n + q][at_] = value

    @pl.when(i < 16)
    def _():
        for q in range(2):
            for n in range(2 * tiles):
                parts = []
                for k in range(4 * n, 4 * n + 4):
                    owner, j = k // tiles, k % tiles
                    parts.append(sgu_ref[0, owner // 4, j, q, :, 32 * (owner % 4) : 32 * (owner % 4) + 32])
                one(q, (0, slice(None), pl.ds(U * n, U)), jnp.concatenate(parts, axis=1))

    @pl.when(i >= 16)
    def _():
        def tile(j, _):
            for k in range(2):
                for h in range(8):
                    at_ = (0, pl.ds(pl.multiple_of(32 * j + 16 * k, 16), 16), pl.ds(U * h, U))
                    one(2, at_, sd_ref[0, 8 * k + h, j, 0])
            return 0

        lax.fori_loop(0, tiles, tile, 0)


def update(sums, weights, m, v):
    _layers, rows, ff = weights[0].shape
    tiles = ff // TN
    gu = pl.BlockSpec((1, 16, ff), lambda i: (jnp.minimum(i, 15) // 8, jnp.minimum(i, 15) % 8, 0))
    down = lambda i: jnp.maximum(i - 16, 0)
    wd = pl.BlockSpec((1, *weights[2].shape[1:]), lambda i: (down(i), 0, 0))
    specs = [gu, gu, wd] * 3
    arrays = (*weights, *m, *v)
    return pl.pallas_call(
        functools.partial(update_kernel, tiles),
        grid=(18,),
        in_specs=[
            pl.BlockSpec((1, 2, tiles, 3, 16, U), lambda i: (jnp.minimum(i, 15) // 8, jnp.minimum(i, 15) % 8, 0, 0, 0, 0)),
            pl.BlockSpec((1, 16, tiles, 1, 16, U), lambda i: (down(i), 0, 0, 2, 0, 0)),
        ]
        + specs,
        out_specs=specs,
        out_shape=[jax.ShapeDtypeStruct(one.shape, one.dtype) for one in arrays],
        compiler_params=pltpu.CompilerParams(vmem_limit_bytes=VMEM_LIMIT),
        name="update",
    )(sums, sums, *arrays)


def solution(mesh):
    def step(x, dy, *arrays):
        weights, m, v = (arrays[i : i + 3] for i in (0, 3, 6))
        early = 5
        s, t, p, h, *whole = forward(x[0], *weights, early)
        sums = backward(x[0], h, dy[0], *whole, s, t, p, early)
        return tuple(update(sums, weights, m, v))

    states, cut = P(("rep", "r", "s"), None, None), P(None, "s", None)
    return jax.shard_map(
        step,
        mesh=mesh,
        in_specs=(states, states) + (cut,) * 9,
        out_specs=(P("rep", "s", None),) * 9,
        check_vma=False,
    )
```

```python
import functools

import jax
import jax.numpy as jnp
from jax import lax
from jax.experimental import pallas as pl
from jax.experimental.pallas import tpu as pltpu
from jax.sharding import PartitionSpec as P

MESH = pl.DeviceIdType.MESH
f32, bf16 = jnp.float32, jnp.bfloat16
TN = 256
MC = 512
U = 128
VMEM_LIMIT = 67043328


def dot(a, b):
    return lax.dot_general(a, b, (((1,), (0,)), ((), ())), preferred_element_type=f32)


def dot_nt(a, b):
    return lax.dot_general(a, b, (((1,), (1,)), ((), ())), preferred_element_type=f32)


def normed(h):
    wide = h.astype(f32)
    scale = lax.rsqrt(jnp.mean(wide**2, -1, keepdims=True) + 1e-6)
    return (wide * scale).astype(bf16)


def chunks(n, step):
    return [pl.ds(i, step) for i in range(0, n, step)]


class Place:
    def __init__(self):
        self.r, self.s = lax.axis_index("r"), lax.axis_index("s")
        self.y, self.z, self.x, self.c = self.r // 4, self.r % 4, self.s // 2, self.s % 2
        self.peer = (0, self.r, self.s + 1 - 2 * self.c)

    def along(self, dim, d):
        if dim == "y":
            return (0, lax.rem(self.y + d, 4) * 4 + self.z, self.s)
        if dim == "z":
            return (0, self.y * 4 + lax.rem(self.z + d, 4), self.s)
        return (0, self.r, lax.rem(self.x + d, 4) * 2 + self.c)


    def partners(self, along_r):
        some = [self.peer] + [self.along("x", d) for d in (1, 2, 3)]
        if along_r:
            return some + [(0, lax.rem(self.r + d, 16), self.s) for d in range(1, 16)]
        return some + [self.along(dim, d) for dim in "yz" for d in (1, 2, 3)]

    def greet(self, along_r=False):
        barrier = pltpu.get_barrier_semaphore()
        for one in self.partners(along_r):
            pl.semaphore_signal(barrier, inc=1, device_id=one, device_id_type=MESH)

    def greeted(self, along_r=False):
        pl.semaphore_wait(pltpu.get_barrier_semaphore(), len(self.partners(along_r)))


def remote(src, dst, ss, rs, dev):
    return pltpu.make_async_remote_copy(src_ref=src, dst_ref=dst, send_sem=ss, recv_sem=rs, device_id=dev, device_id_type=MESH)


class Fetch:
    A, B, D = 288, 864, 1152

    def __init__(self, place, own, whole, some, sends, recvs):
        self.p, self.own, self.whole, self.some, self.sends, self.recvs = place, own, whole, some, sends, recvs

    def quarters(self, refs, *owner):
        p, (wg, wu, wd) = self.p, refs
        every = (slice(None),)
        return (
            (wg.at[(*owner, pl.ds(32 * p.y, 32))], "y"),
            (wu.at[(*owner, pl.ds(32 * p.z, 32))], "z"),
            (wd.at[(*owner, *every, pl.ds(pl.multiple_of(128 * p.y, 128), 128))], "y"),
            (wd.at[(*owner, *every, pl.ds(pl.multiple_of(512 + 128 * p.z, 128), 128))], "z"),
        )

    def wait(self, rows, sem):
        some = self.some.at[pl.ds(0, rows // 32)]
        pltpu.make_async_copy(some, some, sem).wait()

    def a(self, tile, n):
        src = self.quarters(self.own(tile))
        for d in (1, 2, 3):
            dst = self.quarters(self.whole(tile), 4 - d, self.p.c)
            for (one, _), (other, _) in zip(src, dst, strict=True):
                remote(one, other, self.sends.at[0], self.recvs[0].at[n], self.p.along("x", d)).start()

    def b(self, tile, n):
        self.wait(self.A, self.recvs[0].at[n])
        for ref, dim in self.quarters(self.whole(tile), pl.ds(1, 3), self.p.c):
            for d in (1, 2, 3):
                remote(ref, ref, self.sends.at[1], self.recvs[1].at[n], self.p.along(dim, d)).start()

    def d(self, tile, n):
        self.wait(self.B, self.recvs[1].at[n])
        for whole in self.whole(tile):
            ref = whole.at[pl.ds(1, 3), self.p.c]
            remote(ref, ref, self.sends.at[2], self.recvs[2].at[n], self.p.peer).start()

    def here(self, n):
        self.wait(self.D, self.recvs[2].at[n])

    def sent(self, count):
        def one(_n, _):
            for k, rows in enumerate((self.A, self.B, self.D)):
                self.wait(rows, self.sends.at[k])
            return 0

        lax.fori_loop(0, count, one, 0)


def forward_kernel(tiles, early, x_ref, wg_ref, wu_ref, wd_ref, s_ref, t_ref, p_ref, h_ref, at_ref, wg_all, wu_all, wd_all, some_ref,
                   xv, wg_in, wu_in, wd_in, a, at, acc, wgp, wup, tg, tu, td, isem, osem, orecv, lsem, sends, arecv, brecv, drecv):
    k = pl.program_id(0)
    tokens = x_ref.shape[0]
    place = Place()
    count = tiles + early
    fetch = Fetch(
        place,
        lambda n: (wgp.at[n // tiles, lax.rem(n, tiles)], wup.at[n // tiles, lax.rem(n, tiles)], wd_in.at[n // tiles, lax.rem(n, tiles)]),
        lambda n: (wg_all.at[n // tiles, lax.rem(n, tiles)], wu_all.at[n // tiles, lax.rem(n, tiles)], wd_all.at[n // tiles, lax.rem(n, tiles)]),
        some_ref,
        sends,
        (arecv, brecv, drecv),
    )

    def own_copies(n):
        blocks = (
            (wgp.at[n], wg_all.at[n, :, 0, place.c]),
            (wup.at[n], wu_all.at[n, :, 0, place.c]),
            (wd_in.at[n], wd_all.at[n, :, 0, place.c]),
        )
        here = [pltpu.make_async_copy(src, dst, lsem.at[n, m, 0]) for m, (src, dst) in enumerate(blocks)]
        there = [remote(src, dst, osem.at[n, m], orecv.at[n, m], place.peer) for m, (src, dst) in enumerate(blocks)]
        return here + there

    quarter = lax.broadcasted_iota(jnp.int32, (16, U), 1) // 32

    def permute(n):
        def rows_of(i, _):
            rows = pl.ds(pl.multiple_of(16 * i, 16), 16)
            for src, dst in ((wg_in, wgp), (wu_in, wup)):
                for j in range(tiles):
                    for h in range(2):
                        v = None
                        for o in range(4 * h, 4 * h + 4):
                            one = src[n, rows, pl.ds((416 * o + 32 * j) // U * U, U)]
                            v = one if v is None else jnp.where(quarter == (o + j) % 4, one, v)
                        t = 32 * (j % 4)
                        if t:
                            v = jnp.concatenate([v[:, t:], v[:, :t]], axis=1)
                        dst[n, j, rows, U * h : U * h + U] = v
            return 0

        lax.fori_loop(0, 8, rows_of, 0)

    def loads(tile):
        slot = lax.rem(tile, 2)
        copies = []
        for q, (src, dst) in enumerate(((wg_all, tg), (wu_all, tu), (wd_all, td))):
            for e in range(4):
                copies.append(pltpu.make_async_copy(src.at[0, tile, e], dst.at[slot, lax.rem(place.x + e, 4)], lsem.at[2 + slot, q, e]))
        return copies

    def load(tile):
        fetch.here(tile)
        for cp in loads(tile):
            cp.start()

    def out_at():
        return pltpu.make_async_copy(at, at_ref, isem.at[4])

    @pl.when(k == 0)
    def _():
        place.greet()
        ins = ((wg_ref, wg_in), (wu_ref, wu_in), (wd_ref, wd_in), (x_ref, xv))
        copies = [pltpu.make_async_copy(src, dst, isem.at[n]) for n, (src, dst) in enumerate(ins)]
        for cp in copies:
            cp.start()
        for cp in copies[:3]:
            cp.wait()
        permute(0)
        place.greeted()
        for n in range(3):
            fetch.a(n, n)
        for cp in own_copies(0):
            cp.start()
        for n in range(3, 5):
            fetch.a(n, n)
        copies[3].wait()
        for rows in chunks(tokens, 256):
            a[rows, :] = normed(xv[rows, :])
        fetch.b(0, 0)
        fetch.b(1, 1)
        for rows in chunks(tokens, 256):
            at[:, rows] = a[rows, :].T
        out_at().start()
        fetch.d(0, 0)
        fetch.b(2, 2)
        fetch.b(3, 3)
        for cp in own_copies(0):
            cp.wait()
        load(0)

    @pl.when((k >= 2) & (k < tiles - 1))
    def _():
        load(k + 1)

    @pl.when(k >= 2)
    def _():
        @pl.when(k + 5 < count)
        def _():
            fetch.a(k + 5, k + 5)

        fetch.b(k + 4, k + 4)
        fetch.d(k + 2, k + 2)

    slot = lax.rem(k, 2)
    for cp in loads(k):
        cp.wait()
    wg, wu, wd = tg[slot].reshape(-1, TN), tu[slot].reshape(-1, TN), td[slot].reshape(TN, -1)
    for rows in chunks(tokens, MC):
        g = dot(a[rows, :], wg)
        u = dot(a[rows, :], wu)
        sig = jax.nn.sigmoid(g)
        silu = g * sig
        s_ref[rows, :] = silu
        t_ref[rows, :] = u * (sig * (1 + g * (1 - sig)))
        p_ref[rows, :] = (silu * u).astype(bf16)
    for rows in chunks(tokens, MC):
        acc[rows, :] = jnp.where(k == 0, 0.0, acc[rows, :]) + dot(p_ref[rows, :], wd)

    @pl.when(k == 0)
    def _():
        fetch.d(1, 1)
        fetch.b(4, 4)
        fetch.a(5, 5)
        fetch.d(2, 2)
        load(1)

    @pl.when(k == 1)
    def _():
        fetch.d(3, 3)
        load(2)
        fetch.b(5, 5)
        fetch.a(6, 6)

    @pl.when(k == 2)
    def _():
        permute(1)
        for cp in own_copies(1):
            cp.start()

    @pl.when(k == tiles - 1)
    def _():
        for n in range(tiles + 2, count):
            fetch.d(n, n)
        parts = chunks(tokens, 256)
        out_h = [pltpu.make_async_copy(xv.at[rows, :], h_ref.at[rows, :], isem.at[5 + m]) for m, rows in enumerate(parts)]
        for rows, cp in zip(parts, out_h, strict=True):
            xv[rows, :] = xv[rows, :] + acc[rows, :].astype(bf16)
            cp.start()
        for cp in own_copies(1):
            cp.wait()
        for n in range(tiles, count):
            fetch.here(n)
        fetch.sent(count)
        out_at().wait()
        for cp in out_h:
            cp.wait()


def forward(x, wg, wu, wd, early):
    tokens, d = x.shape
    ff = wg.shape[2]
    tiles = ff // TN
    assert early == 4
    anywhere = pl.BlockSpec(memory_space=pl.ANY)
    hid = pl.BlockSpec((tokens, TN), lambda k: (0, k))
    wd = wd.reshape(2, tiles, 32, d)
    dma = pltpu.SemaphoreType.DMA
    return pl.pallas_call(
        functools.partial(forward_kernel, tiles, early),
        grid=(tiles,),
        in_specs=[anywhere] * 4,
        out_specs=[hid, hid, hid] + [anywhere] * 6,
        out_shape=[jax.ShapeDtypeStruct((tokens, ff), f32)] * 2
        + [jax.ShapeDtypeStruct((tokens, ff), bf16), jax.ShapeDtypeStruct((tokens, d), bf16), jax.ShapeDtypeStruct((d, tokens), bf16)]
        + [jax.ShapeDtypeStruct((2, tiles, 4, 2, 128, TN), bf16)] * 2
        + [jax.ShapeDtypeStruct((2, tiles, 4, 2, 32, d), bf16)]
        + [jax.ShapeDtypeStruct((36, 32, TN), bf16)],
        scratch_shapes=[
            pltpu.VMEM((tokens, d), bf16),
            pltpu.VMEM(wg.shape, bf16),
            pltpu.VMEM(wu.shape, bf16),
            pltpu.VMEM(wd.shape, bf16),
            pltpu.VMEM((tokens, d), bf16),
            pltpu.VMEM((d, tokens), bf16),
            pltpu.VMEM((tokens, d), f32),
            pltpu.VMEM((2, tiles, 128, TN), bf16),
            pltpu.VMEM((2, tiles, 128, TN), bf16),
            pltpu.VMEM((2, 4, 2, 128, TN), bf16),
            pltpu.VMEM((2, 4, 2, 128, TN), bf16),
            pltpu.VMEM((2, 4, 2, 32, d), bf16),
            dma((13,)),
            dma((2, 3)),
            dma((2, 3)),
            dma((4, 3, 4)),
            dma((3,)),
            dma((tiles + early,)),
            dma((tiles + early,)),
            dma((tiles + early,)),
        ],
        compiler_params=pltpu.CompilerParams(vmem_limit_bytes=VMEM_LIMIT, has_side_effects=True, collective_id=1),
        cost_estimate=pl.CostEstimate(flops=6 * tokens * d * ff, bytes_accessed=10 * tokens * ff, transcendentals=0),
        name="forward0",
    )(x, wg, wu, wd)


def backward_kernel(tiles, early, at_ref, h_ref, dy_ref, wg_ref, wu_ref, wd_ref, s_ref, t_ref, p_ref,
                    sums_ref, wg_more, wu_more, wd_more, some_ref,
                    a, at, dy, accg, accu, pbuf, dg, du, tg, tu, td, dgu, dwd, r0gu, r0wd, s1, r1, s2, r2, s3, r3, fin, held,
                    lsem, tsem, s0s, s0r, s1s, s1r, s2s, s2r, s3s, s3r, ags, agr, hs, hr, sends, arecv, brecv, drecv):
    i = pl.program_id(0)
    tokens = a.shape[0]
    place = Place()
    r, c = place.r, place.c
    total = 2 * tiles
    where = {"x": place.x, "y": place.y, "z": place.z}
    ORDER = ("yzx", "zxy", "xyz")

    def stage0(tile):
        slot = lax.rem(tile, 2)
        return [
            remote(dgu.at[slot, :, :, 1 - c], r0gu.at[slot], s0s.at[slot, 0], s0r.at[slot, 0], place.peer),
            remote(dwd.at[slot, :, 1 - c], r0wd.at[slot], s0s.at[slot, 1], s0r.at[slot, 1], place.peer),
        ]

    STAGES = ((s1, r1, s1s, s1r, 2, 4), (s2, r2, s2s, s2r, 2, 4), (s3, r3, s3s, s3r, 2, 4))

    def exchange(n, tile):
        src, dst, ss, rs, held, slots = STAGES[n]
        own, slot = lax.rem(tile, held), lax.rem(tile, slots)
        for q in range(3):
            dim = ORDER[q][n]
            for d in (1, 2, 3):
                part = src.at[own, q, lax.rem(where[dim] + d, 4)]
                remote(part, dst.at[slot, q, d - 1], ss.at[own], rs.at[slot], place.along(dim, d)).start()

    def arrived(n, tile):
        src, dst, ss, rs, held, slots = STAGES[n]
        own, slot = lax.rem(tile, held), lax.rem(tile, slots)
        sent = src.at[own, :, pl.ds(0, 3)]
        pltpu.make_async_copy(sent, sent, ss.at[own]).wait()
        pltpu.make_async_copy(dst.at[slot], dst.at[slot], rs.at[slot]).wait()

    def added(n, tile, q):
        src, dst, _ss, _rs, held, slots = STAGES[n]
        slot = lax.rem(tile, slots)
        own = src[lax.rem(tile, held), q, where[ORDER[q][n]]].astype(f32)
        return (own + dst[slot, q, 0].astype(f32) + dst[slot, q, 1].astype(f32) + dst[slot, q, 2].astype(f32)).astype(bf16)

    fetch = Fetch(
        place,
        lambda j: tuple(w.at[1, j, 0, place.c] for w in (wg_ref, wu_ref, wd_ref)),
        lambda j: (wg_more.at[j - early], wu_more.at[j - early], wd_more.at[j - early]),
        some_ref,
        sends,
        (arecv, brecv, drecv),
    )

    def load(tile, act):
        slot = lax.rem(tile, 2)
        for own, some in ((tile < early, lambda w, _more, e: w.at[1, tile, e]), (tile >= early, lambda w, more, e: more.at[tile - early, e] if e else w.at[1, tile, e])):

            @pl.when(own)
            def _(some=some):
                for q, (w, more, dst) in enumerate(((wg_ref, wg_more, tg), (wu_ref, wu_more, tu), (wd_ref, wd_more, td))):
                    for e in range(4):
                        act(pltpu.make_async_copy(some(w, more, e), dst.at[slot, lax.rem(place.x + e, 4)], tsem.at[slot, q, e]))

    def load0(tile, act):
        slot = lax.rem(tile, 2)
        for e in range(4):
            act(pltpu.make_async_copy(wd_ref.at[0, tile - tiles, e], td.at[slot, lax.rem(place.x + e, 4)], tsem.at[slot, 2, e]))

    @pl.when(i == 0)
    def _():
        place.greet(True)
        cp = [pltpu.make_async_copy(h_ref, a, lsem.at[0]), pltpu.make_async_copy(dy_ref, dy, lsem.at[1])]
        cp[0].start()
        cp[1].start()
        load(i, lambda cp: cp.start())
        cp[0].wait()
        for rows in chunks(tokens, 256):
            v = normed(a[rows, :])
            a[rows, :] = v
            at[:, rows] = v.T
        cp[1].wait()
        place.greeted(True)
        fetch.a(early, 0)

    @pl.when((i >= early - 1) & (i < tiles - 1))
    def _():
        fetch.here(i + 1 - early)

    @pl.when(i < tiles - 1)
    def _():
        load(i + 1, lambda cp: cp.start())

    @pl.when((i >= tiles - 1) & (i < total - 1))
    def _():
        load0(i + 1, lambda cp: cp.start())

    def by_weights(p):
        slot = lax.rem(i, 2)
        for q, one in ((0, dg), (1, du)):
            dgu[slot, q] = dot(at[...], one[...]).astype(bf16).reshape(dgu.shape[2:])
        dwd[slot] = dot(p[...].T, dy[...]).astype(bf16).reshape(dwd.shape[1:])

    @pl.when(i < tiles)
    def _():
        slot = lax.rem(i, 2)
        load(i, lambda cp: cp.wait())
        wg, wu, wd = tg[slot].reshape(-1, TN), tu[slot].reshape(-1, TN), td[slot].reshape(TN, -1)
        for rows in chunks(tokens, MC):
            g = dot(a[rows, :], wg)
            u = dot(a[rows, :], wu)
            d = dot_nt(dy[rows, :], wd).astype(bf16).astype(f32)
            sig = jax.nn.sigmoid(g)
            silu = g * sig
            pbuf[rows, :] = (silu * u).astype(bf16)
            du[rows, :] = (d * silu).astype(bf16)
            dg[rows, :] = (d * u * (sig * (1 + g * (1 - sig)))).astype(bf16)
        for rows in chunks(tokens, MC):
            accg[rows, :] = jnp.where(i == 0, 0.0, accg[rows, :]) + dot_nt(dg[rows, :], wg)
            accu[rows, :] = jnp.where(i == 0, 0.0, accu[rows, :]) + dot_nt(du[rows, :], wu)
        by_weights(pbuf)

    @pl.when((i >= tiles) & (i < total))
    def _():
        load0(i, lambda cp: cp.wait())
        wd = td[lax.rem(i, 2)].reshape(TN, -1)
        for rows in chunks(tokens, MC):
            d = dot_nt(dy[rows, :], wd).astype(bf16).astype(f32)
            du[rows, :] = (d * s_ref[rows, :]).astype(bf16)
            dg[rows, :] = (d * t_ref[rows, :]).astype(bf16)
        by_weights(p_ref)

    @pl.when(i == tiles - 1)
    def _():
        pltpu.make_async_copy(h_ref, a, lsem.at[0]).start()

    def spread(tile):
        layer, j = 1 - tile // tiles, lax.rem(tile, tiles)
        src, dst = fin.at[tile], sums_ref.at[layer, place.y, place.z, j]
        pltpu.make_async_copy(src, dst, agr.at[0]).start()

        def one(d, _):
            to = lax.rem(r + d, 16)
            remote(src, dst, ags.at[0], agr.at[0], (0, to, place.s)).start()
            return 0

        lax.fori_loop(1, 16, one, 0)

    def first_half(tile):
        slot = lax.rem(tile, 4)
        for k, dim in enumerate("yz"):

            @pl.when(lax.rem(tile, 2) == k)
            def _(k=k, dim=dim):
                me = where[dim]
                for q in range(3):
                    held[slot, me, q] = fin[tile, q]
                for d in (1, 2, 3):
                    remote(fin.at[tile], held.at[slot, me], hs.at[k], hr.at[slot], place.along(dim, d)).start()

    def passed_on():
        pltpu.make_async_copy(held.at[0], held.at[0], hs.at[2]).wait()
        pltpu.make_async_copy(held.at[pl.ds(0, 3)], held.at[pl.ds(0, 3)], hs.at[3]).wait()

    def second_half(tile):
        layer, j, slot = 1 - tile // tiles, lax.rem(tile, tiles), lax.rem(tile, 4)
        three = held.at[slot, pl.ds(0, 3)]
        pltpu.make_async_copy(three, three, hr.at[slot]).wait()
        pltpu.make_async_copy(three, three, hs.at[lax.rem(tile, 2)]).wait()

        @pl.when(tile > 0)
        def _():
            passed_on()

        for k, dim in enumerate("yz"):

            @pl.when(lax.rem(tile, 2) == k)
            def _(dim=dim):
                other = "z" if dim == "y" else "y"
                dst = sums_ref.at[layer, :, place.z, j] if dim == "y" else sums_ref.at[layer, place.y, :, j]
                pltpu.make_async_copy(held.at[slot], dst, hs.at[2]).start()
                for d in (1, 2, 3):
                    remote(held.at[slot], dst, hs.at[3], agr.at[0], place.along(other, d)).start()

    def stage4(tile):
        arrived(2, tile)
        for q in range(3):
            fin[tile, q] = added(2, tile, q)

        @pl.when(tile < total - 2)
        def _():
            first_half(tile)

        @pl.when(tile >= total - 2)
        def _():
            spread(tile)

    def stage3(tile):
        arrived(1, tile)
        for q in range(3):
            s3[lax.rem(tile, 2), q] = added(1, tile, q)
        exchange(2, tile)

    def stage2(tile):
        arrived(0, tile)
        for q in range(3):
            s2[lax.rem(tile, 2), q] = added(0, tile, q)
        exchange(1, tile)

    for stage, lag in ((stage4, 5), (stage3, 4), (stage2, 3)):
        end = total + lag - 1

        def steps(first, stage=stage, lag=lag, end=end):
            count = jnp.where(first == end - 1, 2, 1)

            def one(n, _):
                stage(first - lag + n)
                return 0

            lax.fori_loop(0, count, one, 0)

        @pl.when((i >= lag) & (i < end))
        def _(steps=steps):
            steps(i)

    @pl.when((i >= 1) & (i < total + 1))
    def _():
        tile = i - 1
        slot = lax.rem(tile, 2)
        for cp in stage0(tile):
            cp.wait()
        for xi in range(4):
            for k in range(8):
                for h in range(2):
                    rows, cols = pl.ds(16 * k, 16), pl.ds(U * h, U)
                    yi, zi = k // 2, 2 * (k % 2) + h
                    for q, at_ in ((0, (yi, zi, xi)), (1, (zi, xi, yi))):
                        v = dgu[slot, q, xi, c, rows, cols].astype(f32) + r0gu[slot, q, xi, rows, cols].astype(f32)
                        s1[(slot, q, *at_)] = v.astype(bf16)
                    rows, cols = pl.ds(16 * (yi // 2), 16), pl.ds(U * (4 * (yi % 2) + zi), U)
                    v = dwd[slot, xi, c, rows, cols].astype(f32) + r0wd[slot, xi, rows, cols].astype(f32)
                    s1[slot, 2, xi, yi, zi] = v.astype(bf16)
        exchange(0, tile)

    @pl.when(i < total)
    def _():
        for cp in stage0(i):
            cp.start()

    @pl.when(i == 0)
    def _():
        for tile in range(early + 1, tiles):
            fetch.a(tile, tile - early)

    @pl.when((i + 3 >= early) & (i + 3 < tiles))
    def _():
        fetch.d(i + 3, i + 3 - early)

    @pl.when((i + 4 >= early) & (i + 4 < tiles))
    def _():
        fetch.b(i + 4, i + 4 - early)

    @pl.when((i >= 6) & (i < total + 4))
    def _():
        second_half(i - 6)

    @pl.when(i == tiles - 1)
    def _():
        pltpu.make_async_copy(h_ref, a, lsem.at[0]).wait()
        new_at = pltpu.make_async_copy(at_ref, at, lsem.at[1])
        new_at.start()

        def some(k, _):
            rows = pl.ds(pl.multiple_of(32 * k, 32), 32)
            da = (accg[rows, :].astype(bf16) + accu[rows, :].astype(bf16)).astype(f32)
            wide = a[rows, :].astype(f32)
            scale = lax.rsqrt(jnp.mean(wide**2, -1, keepdims=True) + 1e-6)
            along = jnp.sum(da * wide, -1, keepdims=True)
            by_h = da * scale - wide * (along * (scale * scale * scale) * (1.0 / wide.shape[-1]))
            dy[rows, :] = dy[rows, :] + by_h.astype(bf16)
            return 0

        lax.fori_loop(0, tokens // 32, some, 0, unroll=4)
        new_at.wait()

    @pl.when(i == total + 3)
    def _():
        fetch.sent(tiles - early)
        passed_on()
        for units, sem in ((2 * 15 * 3, ags.at[0]), ((total - 2) * 36 + 2 * 48, agr.at[0])):
            some = some_ref.at[pl.ds(0, units // 4)] if units % 4 == 0 else some_ref.at[pl.ds(0, units // 2), pl.ds(0, 16)]
            pltpu.make_async_copy(some, some, sem).wait()


def backward(at, h, dy, wg, wu, wd, s, t, p, early):
    tokens, d = h.shape
    ff = s.shape[1]
    tiles = ff // TN
    last = tiles - 1
    anywhere = pl.BlockSpec(memory_space=pl.ANY)
    clamp = lambda i: jnp.clip(i - tiles, 0, last)
    hid = pl.BlockSpec((tokens, TN), lambda i: (0, clamp(i)))
    dma = pltpu.SemaphoreType.DMA
    unit = (16, U)
    return pl.pallas_call(
        functools.partial(backward_kernel, tiles, early),
        grid=(2 * tiles + 4,),
        in_specs=[anywhere] * 6 + [hid] * 3,
        out_specs=[anywhere] * 5,
        out_shape=[
            jax.ShapeDtypeStruct((2, 4, 4, tiles, 3, *unit), bf16),
            jax.ShapeDtypeStruct((tiles - early, 4, 2, 128, TN), bf16),
            jax.ShapeDtypeStruct((tiles - early, 4, 2, 128, TN), bf16),
            jax.ShapeDtypeStruct((tiles - early, 4, 2, 32, d), bf16),
            jax.ShapeDtypeStruct((240, 32, TN), bf16),
        ],
        scratch_shapes=[
            pltpu.VMEM((tokens, d), bf16),
            pltpu.VMEM((d, tokens), bf16),
            pltpu.VMEM((tokens, d), bf16),
            pltpu.VMEM((tokens, d), f32),
            pltpu.VMEM((tokens, d), f32),
            pltpu.VMEM((tokens, TN), bf16),
            pltpu.VMEM((tokens, TN), bf16),
            pltpu.VMEM((tokens, TN), bf16),
            pltpu.VMEM((2, 4, 2, 128, TN), bf16),
            pltpu.VMEM((2, 4, 2, 128, TN), bf16),
            pltpu.VMEM((2, 4, 2, 32, d), bf16),
            pltpu.VMEM((2, 2, 4, 2, 128, TN), bf16),
            pltpu.VMEM((2, 4, 2, 32, d), bf16),
            pltpu.VMEM((2, 2, 4, 128, TN), bf16),
            pltpu.VMEM((2, 4, 32, d), bf16),
            pltpu.VMEM((2, 3, 4, 4, 4, *unit), bf16),
            pltpu.VMEM((4, 3, 3, 4, 4, *unit), bf16),
            pltpu.VMEM((2, 3, 4, 4, *unit), bf16),
            pltpu.VMEM((4, 3, 3, 4, *unit), bf16),
            pltpu.VMEM((2, 3, 4, *unit), bf16),
            pltpu.VMEM((4, 3, 3, *unit), bf16),
            pltpu.VMEM((2 * tiles, 3, *unit), bf16),
            pltpu.VMEM((4, 4, 3, *unit), bf16),
            dma((2,)),
            dma((2, 3, 4)),
            dma((2, 2)),
            dma((2, 2)),
            dma((2,)),
            dma((4,)),
            dma((2,)),
            dma((4,)),
            dma((2,)),
            dma((4,)),
            dma((1,)),
            dma((1,)),
            dma((4,)),
            dma((4,)),
            dma((3,)),
            dma((tiles - early,)),
            dma((tiles - early,)),
            dma((tiles - early,)),
        ],
        compiler_params=pltpu.CompilerParams(vmem_limit_bytes=VMEM_LIMIT, has_side_effects=True, collective_id=2),
        cost_estimate=pl.CostEstimate(flops=24 * tokens * d * ff, bytes_accessed=10 * tokens * ff, transcendentals=0),
        name="backward",
    )(at, h, dy, wg, wu, wd, s, t, p)[0]


def adamw(w, m, v, g):
    m = 0.9 * m + 0.1 * g
    v = 0.95 * v + 0.05 * g * g
    step = m * lax.rsqrt(v + 1e-8) + 0.1 * w
    return (w - 0.02 * step).astype(bf16), m, v


ROWS = 64


def update_kernel(tiles, steps, sgu_ref, sd_ref, *refs):
    ins, outs = refs[:9], refs[9:]
    i = pl.program_id(0)

    def one(q, at_, g):
        new = adamw(ins[q][at_].astype(f32), ins[3 + q][at_], ins[6 + q][at_], g.astype(f32))
        for n, value in enumerate(new):
            outs[3 * n + q][at_] = value

    @pl.when(i < steps)
    def _():
        def some(t, _):
            rows = pl.ds(pl.multiple_of(16 * t, 16), 16)
            for q in range(2):
                for n in range(2 * tiles):
                    parts = []
                    for k in range(4 * n, 4 * n + 4):
                        owner, j = k // tiles, k % tiles
                        parts.append(sgu_ref[0, 2 * t + owner // 4, j, q, :, 32 * (owner % 4) : 32 * (owner % 4) + 32])
                    one(q, (0, rows, pl.ds(U * n, U)), jnp.concatenate(parts, axis=1))
            return 0

        lax.fori_loop(0, ROWS // 16, some, 0)

    @pl.when(i >= steps)
    def _():
        def tile(j, _):
            for k in range(2):
                for h in range(8):
                    at_ = (0, pl.ds(pl.multiple_of(32 * j + 16 * k, 16), 16), pl.ds(U * h, U))
                    one(2, at_, sd_ref[0, 8 * k + h, j, 0])
            return 0

        lax.fori_loop(0, tiles, tile, 0)


def update(sums, weights, m, v):
    layers, rows, ff = weights[0].shape
    tiles = ff // TN
    each = rows // ROWS
    steps = layers * each
    here = lambda i: (jnp.minimum(i, steps - 1) // each, jnp.minimum(i, steps - 1) % each)
    gu = pl.BlockSpec((1, ROWS, ff), lambda i: (*here(i), 0))
    down = lambda i: jnp.maximum(i - steps, 0)
    wd = pl.BlockSpec((1, *weights[2].shape[1:]), lambda i: (down(i), 0, 0))
    specs = [gu, gu, wd] * 3
    arrays = (*weights, *m, *v)
    return pl.pallas_call(
        functools.partial(update_kernel, tiles, steps),
        grid=(steps + layers,),
        in_specs=[
            pl.BlockSpec((1, ROWS // 8, tiles, 3, 16, U), lambda i: (*here(i), 0, 0, 0, 0)),
            pl.BlockSpec((1, 16, tiles, 1, 16, U), lambda i: (down(i), 0, 0, 2, 0, 0)),
        ]
        + specs,
        out_specs=specs,
        out_shape=[jax.ShapeDtypeStruct(one.shape, one.dtype) for one in arrays],
        compiler_params=pltpu.CompilerParams(vmem_limit_bytes=VMEM_LIMIT),
        name="update",
    )(sums, sums, *arrays)


def solution(mesh):
    def step(x, dy, *arrays):
        weights, m, v = (arrays[i : i + 3] for i in (0, 3, 6))
        early = 4
        s, t, p, h, at, *whole, _ = forward(x[0], *weights, early)
        sums = backward(at, h, dy[0], *whole, s, t, p, early)
        sums = sums.reshape(2, 16, *sums.shape[3:])
        return tuple(update(sums, weights, m, v))

    states, cut = P(("rep", "r", "s"), None, None), P(None, "s", None)
    return jax.shard_map(
        step,
        mesh=mesh,
        in_specs=(states, states) + (cut,) * 9,
        out_specs=(P("rep", "s", None),) * 9,
        check_vma=False,
    )
```

```python
import functools

import jax
import jax.numpy as jnp
from jax import lax
from jax.experimental import pallas as pl
from jax.experimental.pallas import tpu as pltpu
from jax.sharding import PartitionSpec as P

MESH = pl.DeviceIdType.MESH
f32, bf16 = jnp.float32, jnp.bfloat16
TN = 256
MC = 512
U = 128
VMEM_LIMIT = 67043328


def dot(a, b):
    return lax.dot_general(a, b, (((1,), (0,)), ((), ())), preferred_element_type=f32)


def dot_nt(a, b):
    return lax.dot_general(a, b, (((1,), (1,)), ((), ())), preferred_element_type=f32)


def normed(h):
    wide = h.astype(f32)
    scale = lax.rsqrt(jnp.mean(wide**2, -1, keepdims=True) + 1e-6)
    return (wide * scale).astype(bf16)


def chunks(n, step):
    return [pl.ds(i, step) for i in range(0, n, step)]


class Place:
    def __init__(self):
        self.r, self.s = lax.axis_index("r"), lax.axis_index("s")
        self.y, self.z, self.x, self.c = self.r // 4, self.r % 4, self.s // 2, self.s % 2
        self.peer = (0, self.r, self.s + 1 - 2 * self.c)

    def along(self, dim, d):
        if dim == "y":
            return (0, lax.rem(self.y + d, 4) * 4 + self.z, self.s)
        if dim == "z":
            return (0, self.y * 4 + lax.rem(self.z + d, 4), self.s)
        return (0, self.r, lax.rem(self.x + d, 4) * 2 + self.c)


    def partners(self, along_r):
        some = [self.peer] + [self.along("x", d) for d in (1, 2, 3)]
        if along_r:
            return some + [(0, lax.rem(self.r + d, 16), self.s) for d in range(1, 16)]
        return some + [self.along(dim, d) for dim in "yz" for d in (1, 2, 3)]

    def greet(self, along_r=False):
        barrier = pltpu.get_barrier_semaphore()
        for one in self.partners(along_r):
            pl.semaphore_signal(barrier, inc=1, device_id=one, device_id_type=MESH)

    def greeted(self, along_r=False):
        pl.semaphore_wait(pltpu.get_barrier_semaphore(), len(self.partners(along_r)))


def remote(src, dst, ss, rs, dev):
    return pltpu.make_async_remote_copy(src_ref=src, dst_ref=dst, send_sem=ss, recv_sem=rs, device_id=dev, device_id_type=MESH)


class Fetch:
    A, B = 288, 864

    def __init__(self, place, own, whole, some, sends, recvs, first):
        self.p, self.own, self.whole, self.some, self.sends, self.recvs = place, own, whole, some, sends, recvs
        self.handed = pl.ds(first, 4 - first)
        self.D = 384 * (4 - first)

    def quarters(self, refs, *owner):
        p, (wg, wu, wd) = self.p, refs
        every = (slice(None),)
        return (
            (wg.at[(*owner, pl.ds(32 * p.y, 32))], "y"),
            (wu.at[(*owner, pl.ds(32 * p.z, 32))], "z"),
            (wd.at[(*owner, *every, pl.ds(pl.multiple_of(128 * p.y, 128), 128))], "y"),
            (wd.at[(*owner, *every, pl.ds(pl.multiple_of(512 + 128 * p.z, 128), 128))], "z"),
        )

    def wait(self, rows, sem):
        some = self.some.at[pl.ds(0, rows // 32)]
        pltpu.make_async_copy(some, some, sem).wait()

    def a(self, tile, n):
        src = self.quarters(self.own(tile))
        for d in (1, 2, 3):
            dst = self.quarters(self.whole(tile), 4 - d, self.p.c)
            for (one, _), (other, _) in zip(src, dst, strict=True):
                remote(one, other, self.sends.at[0], self.recvs[0].at[n], self.p.along("x", d)).start()

    def b(self, tile, n):
        self.wait(self.A, self.recvs[0].at[n])
        for ref, dim in self.quarters(self.whole(tile), pl.ds(1, 3), self.p.c):
            for d in (1, 2, 3):
                remote(ref, ref, self.sends.at[1], self.recvs[1].at[n], self.p.along(dim, d)).start()

    def d(self, tile, n):
        self.wait(self.B, self.recvs[1].at[n])
        for whole in self.whole(tile):
            ref = whole.at[self.handed, self.p.c]
            remote(ref, ref, self.sends.at[2], self.recvs[2].at[n], self.p.peer).start()

    def here(self, n):
        self.wait(self.D, self.recvs[2].at[n])

    def sent(self, count):
        def one(_n, _):
            for k, rows in enumerate((self.A, self.B, self.D)):
                self.wait(rows, self.sends.at[k])
            return 0

        lax.fori_loop(0, count, one, 0)


def forward_kernel(tiles, early, x_ref, wg_ref, wu_ref, wd_ref, s_ref, t_ref, p_ref, h_ref, at_ref, wg_all, wu_all, wd_all, some_ref,
                   xv, wg_in, wu_in, wd_in, a, at, acc, wgp, wup, tg, tu, td, isem, osem, orecv, lsem, sends, arecv, brecv, drecv):
    k = pl.program_id(0)
    tokens = x_ref.shape[0]
    place = Place()
    count = tiles + early
    fetch = Fetch(
        place,
        lambda n: (wgp.at[n // tiles, lax.rem(n, tiles)], wup.at[n // tiles, lax.rem(n, tiles)], wd_in.at[n // tiles, lax.rem(n, tiles)]),
        lambda n: (wg_all.at[n // tiles, lax.rem(n, tiles)], wu_all.at[n // tiles, lax.rem(n, tiles)], wd_all.at[n // tiles, lax.rem(n, tiles)]),
        some_ref,
        sends,
        (arecv, brecv, drecv),
        0,
    )

    def own_copies(n):
        blocks = ((wgp.at[n], wg_all.at[n, :, 0, place.c]), (wup.at[n], wu_all.at[n, :, 0, place.c]), (wd_in.at[n], wd_all.at[n, :, 0, place.c]))
        copies = [pltpu.make_async_copy(src, dst, lsem.at[n, m, 0]) for m, (src, dst) in enumerate(blocks)]
        if n == 1:
            late = pl.ds(early, tiles - early)
            copies += [remote(src.at[late], dst.at[late], osem.at[m], orecv.at[m], place.peer) for m, (src, dst) in enumerate(blocks)]
        return copies

    quarter = lax.broadcasted_iota(jnp.int32, (16, U), 1) // 32

    def permute(n):
        def rows_of(i, _):
            rows = pl.ds(pl.multiple_of(16 * i, 16), 16)
            for src, dst in ((wg_in, wgp), (wu_in, wup)):
                for j in range(tiles):
                    for h in range(2):
                        v = None
                        for o in range(4 * h, 4 * h + 4):
                            one = src[n, rows, pl.ds((416 * o + 32 * j) // U * U, U)]
                            v = one if v is None else jnp.where(quarter == (o + j) % 4, one, v)
                        t = 32 * (j % 4)
                        if t:
                            v = jnp.concatenate([v[:, t:], v[:, :t]], axis=1)
                        dst[n, j, rows, U * h : U * h + U] = v
            return 0

        lax.fori_loop(0, 8, rows_of, 0)

    def loads(tile):
        slot = lax.rem(tile, 2)
        copies = []
        for q, (src, dst) in enumerate(((wg_all, tg), (wu_all, tu), (wd_all, td))):
            for e in range(4):
                copies.append(pltpu.make_async_copy(src.at[0, tile, e], dst.at[slot, lax.rem(place.x + e, 4)], lsem.at[2 + slot, q, e]))
        return copies

    def load(tile):
        fetch.here(tile)
        for cp in loads(tile):
            cp.start()

    def fetched(n):
        pairs = ((wg_ref, wg_in), (wu_ref, wu_in), (wd_ref, wd_in))
        return [pltpu.make_async_copy(src.at[n], dst.at[n], isem.at[13 * n + m]) for m, (src, dst) in enumerate(pairs)]

    def out_at():
        return pltpu.make_async_copy(at, at_ref, isem.at[4])

    @pl.when(k == 0)
    def _():
        place.greet()
        for cp in fetched(0):
            cp.start()
        get_x = pltpu.make_async_copy(x_ref, xv, isem.at[3])
        get_x.start()
        for cp in fetched(1):
            cp.start()
        for cp in fetched(0):
            cp.wait()
        permute(0)
        place.greeted()
        for n in range(3):
            fetch.a(n, n)
        for cp in own_copies(0):
            cp.start()
        for n in range(3, 5):
            fetch.a(n, n)
        get_x.wait()
        for rows in chunks(tokens, 256):
            a[rows, :] = normed(xv[rows, :])
        fetch.b(0, 0)
        fetch.b(1, 1)
        for rows in chunks(tokens, 256):
            at[:, rows] = a[rows, :].T
        out_at().start()
        for cp in own_copies(0):
            cp.wait()
        fetch.d(0, 0)
        fetch.b(2, 2)
        fetch.b(3, 3)
        load(0)

    @pl.when((k >= 2) & (k < tiles - 1))
    def _():
        load(k + 1)

    def ahead(stage, lead, more):
        @pl.when((k >= 2) & (k <= more))
        def _():
            stage(k + lead, k + lead)

        @pl.when((k >= more) & (k + lead + 1 < count))
        def _():
            stage(k + lead + 1, k + lead + 1)

    ahead(fetch.a, 5, 6)
    ahead(fetch.b, 4, 8)
    ahead(fetch.d, 2, 10)

    slot = lax.rem(k, 2)
    for cp in loads(k):
        cp.wait()
    wg, wu, wd = tg[slot].reshape(-1, TN), tu[slot].reshape(-1, TN), td[slot].reshape(TN, -1)
    for rows in chunks(tokens, MC):
        g = dot(a[rows, :], wg)
        u = dot(a[rows, :], wu)
        sig = jax.nn.sigmoid(g)
        silu = g * sig
        s_ref[rows, :] = silu
        t_ref[rows, :] = u * (sig * (1 + g * (1 - sig)))
        p_ref[rows, :] = (silu * u).astype(bf16)
    for rows in chunks(tokens, MC):
        acc[rows, :] = jnp.where(k == 0, 0.0, acc[rows, :]) + dot(p_ref[rows, :], wd)

    @pl.when(k == 0)
    def _():
        fetch.d(1, 1)
        fetch.b(4, 4)
        fetch.a(5, 5)
        fetch.d(2, 2)
        load(1)

    @pl.when(k == 1)
    def _():
        fetch.d(3, 3)
        load(2)
        fetch.b(5, 5)
        fetch.a(6, 6)

    @pl.when(k == 2)
    def _():
        for cp in fetched(1):
            cp.wait()
        permute(1)

    @pl.when(k == 6)
    def _():
        for cp in own_copies(1):
            cp.start()

    @pl.when(k == 8)
    def _():
        for cp in own_copies(1):
            cp.wait()

    @pl.when(k == tiles - 1)
    def _():
        fetch.d(count - 1, count - 1)
        parts = chunks(tokens, 256)
        out_h = [pltpu.make_async_copy(xv.at[rows, :], h_ref.at[rows, :], isem.at[5 + m]) for m, rows in enumerate(parts)]
        for rows, cp in zip(parts, out_h, strict=True):
            xv[rows, :] = xv[rows, :] + acc[rows, :].astype(bf16)
            cp.start()
        for n in range(tiles, count):
            fetch.here(n)
        fetch.sent(count)
        out_at().wait()
        for cp in out_h:
            cp.wait()


def forward(x, wg, wu, wd, early):
    tokens, d = x.shape
    ff = wg.shape[2]
    tiles = ff // TN
    assert early == 4
    anywhere = pl.BlockSpec(memory_space=pl.ANY)
    hid = pl.BlockSpec((tokens, TN), lambda k: (0, k))
    wd = wd.reshape(2, tiles, 32, d)
    dma = pltpu.SemaphoreType.DMA
    return pl.pallas_call(
        functools.partial(forward_kernel, tiles, early),
        grid=(tiles,),
        in_specs=[anywhere] * 4,
        out_specs=[hid, hid, hid] + [anywhere] * 6,
        out_shape=[jax.ShapeDtypeStruct((tokens, ff), f32)] * 2
        + [jax.ShapeDtypeStruct((tokens, ff), bf16), jax.ShapeDtypeStruct((tokens, d), bf16), jax.ShapeDtypeStruct((d, tokens), bf16)]
        + [jax.ShapeDtypeStruct((2, tiles, 4, 2, 128, TN), bf16)] * 2
        + [jax.ShapeDtypeStruct((2, tiles, 4, 2, 32, d), bf16)]
        + [jax.ShapeDtypeStruct((48, 32, TN), bf16)],
        scratch_shapes=[
            pltpu.VMEM((tokens, d), bf16),
            pltpu.VMEM(wg.shape, bf16),
            pltpu.VMEM(wu.shape, bf16),
            pltpu.VMEM(wd.shape, bf16),
            pltpu.VMEM((tokens, d), bf16),
            pltpu.VMEM((d, tokens), bf16),
            pltpu.VMEM((tokens, d), f32),
            pltpu.VMEM((2, tiles, 128, TN), bf16),
            pltpu.VMEM((2, tiles, 128, TN), bf16),
            pltpu.VMEM((2, 4, 2, 128, TN), bf16),
            pltpu.VMEM((2, 4, 2, 128, TN), bf16),
            pltpu.VMEM((2, 4, 2, 32, d), bf16),
            dma((16,)),
            dma((3,)),
            dma((3,)),
            dma((4, 3, 4)),
            dma((3,)),
            dma((tiles + early,)),
            dma((tiles + early,)),
            dma((tiles + early,)),
        ],
        compiler_params=pltpu.CompilerParams(vmem_limit_bytes=VMEM_LIMIT, has_side_effects=True, collective_id=1),
        cost_estimate=pl.CostEstimate(flops=6 * tokens * d * ff, bytes_accessed=10 * tokens * ff, transcendentals=0),
        name="forward0",
    )(x, wg, wu, wd)


def backward_kernel(tiles, early, at_ref, h_ref, dy_ref, wg_ref, wu_ref, wd_ref, s_ref, t_ref, p_ref,
                    sums_ref, wg_more, wu_more, wd_more, some_ref,
                    a, at, dy, accg, accu, pbuf, dg, du, tg, tu, td, sv, tv, pv, dgu, dwd, r0gu, r0wd, s1, r1, s2, r2, s3, r3, fin, held,
                    lsem, tsem, hsem, s0s, s0r, s1s, s1r, s2s, s2r, s3s, s3r, ags, agr, hs, hr, sends, arecv, brecv, drecv):
    i = pl.program_id(0)
    tokens = a.shape[0]
    place = Place()
    r, c = place.r, place.c
    total = 2 * tiles
    where = {"x": place.x, "y": place.y, "z": place.z}
    ORDER = ("yzx", "zxy", "xyz")

    def stage0(tile):
        slot = lax.rem(tile, 2)
        return [
            remote(dgu.at[slot, :, :, 1 - c], r0gu.at[slot], s0s.at[slot, 0], s0r.at[slot, 0], place.peer),
            remote(dwd.at[slot, :, 1 - c], r0wd.at[slot], s0s.at[slot, 1], s0r.at[slot, 1], place.peer),
        ]

    STAGES = ((s1, r1, s1s, s1r, 2, 4), (s2, r2, s2s, s2r, 2, 4), (s3, r3, s3s, s3r, 2, 4))

    def exchange(n, tile):
        src, dst, ss, rs, held, slots = STAGES[n]
        own, slot = lax.rem(tile, held), lax.rem(tile, slots)
        for q in range(3):
            dim = ORDER[q][n]
            for d in (1, 2, 3):
                part = src.at[own, q, lax.rem(where[dim] + d, 4)]
                remote(part, dst.at[slot, q, d - 1], ss.at[own], rs.at[slot], place.along(dim, d)).start()

    def arrived(n, tile):
        src, dst, ss, rs, held, slots = STAGES[n]
        own, slot = lax.rem(tile, held), lax.rem(tile, slots)
        sent = src.at[own, :, pl.ds(0, 3)]
        pltpu.make_async_copy(sent, sent, ss.at[own]).wait()
        pltpu.make_async_copy(dst.at[slot], dst.at[slot], rs.at[slot]).wait()

    def added(n, tile, q):
        src, dst, _ss, _rs, held, slots = STAGES[n]
        slot = lax.rem(tile, slots)
        own = src[lax.rem(tile, held), q, where[ORDER[q][n]]].astype(f32)
        return (own + dst[slot, q, 0].astype(f32) + dst[slot, q, 1].astype(f32) + dst[slot, q, 2].astype(f32)).astype(bf16)

    fetch = Fetch(
        place,
        lambda j: tuple(w.at[1, j, 0, place.c] for w in (wg_ref, wu_ref, wd_ref)),
        lambda j: (wg_more.at[j - early], wu_more.at[j - early], wd_more.at[j - early]),
        some_ref,
        sends,
        (arecv, brecv, drecv),
        1,
    )

    def load(tile, act):
        slot = lax.rem(tile, 2)
        for own, some in ((tile < early, lambda w, _more, e: w.at[1, tile, e]), (tile >= early, lambda w, more, e: more.at[tile - early, e] if e else w.at[1, tile, e])):

            @pl.when(own)
            def _(some=some):
                for q, (w, more, dst) in enumerate(((wg_ref, wg_more, tg), (wu_ref, wu_more, tu), (wd_ref, wd_more, td))):
                    for e in range(4):
                        act(pltpu.make_async_copy(some(w, more, e), dst.at[slot, lax.rem(place.x + e, 4)], tsem.at[slot, q, e]))

    def load0(tile, act):
        slot = lax.rem(tile, 2)
        for e in range(4):
            act(pltpu.make_async_copy(wd_ref.at[0, tile - tiles, e], td.at[slot, lax.rem(place.x + e, 4)], tsem.at[slot, 2, e]))
        cols = pl.ds(pl.multiple_of(TN * (tile - tiles), TN), TN)
        for q, (src, dst) in enumerate(((s_ref, sv), (t_ref, tv), (p_ref, pv))):
            act(pltpu.make_async_copy(src.at[:, cols], dst.at[slot], hsem.at[slot, q]))

    @pl.when(i == 0)
    def _():
        place.greet(True)
        parts = chunks(tokens, 256)
        copies = [pltpu.make_async_copy(h_ref.at[rows, :], a.at[rows, :], lsem.at[2 + n]) for n, rows in enumerate(parts)]
        for cp in copies:
            cp.start()
        get_dy = pltpu.make_async_copy(dy_ref, dy, lsem.at[1])
        get_dy.start()
        load(i, lambda cp: cp.start())
        for rows, cp in zip(parts, copies, strict=True):
            cp.wait()
            v = normed(a[rows, :])
            a[rows, :] = v
            at[:, rows] = v.T
        get_dy.wait()
        place.greeted(True)
        fetch.a(early, 0)

    @pl.when((i >= early - 1) & (i < tiles - 1))
    def _():
        fetch.here(i + 1 - early)

    @pl.when(i < tiles - 1)
    def _():
        load(i + 1, lambda cp: cp.start())

    @pl.when((i >= tiles - 1) & (i < total - 1))
    def _():
        load0(i + 1, lambda cp: cp.start())

    def by_weights(p):
        slot = lax.rem(i, 2)
        for q, one in ((0, dg), (1, du)):
            dgu[slot, q] = dot(at[...], one[...]).astype(bf16).reshape(dgu.shape[2:])
        dwd[slot] = dot(p[...].T, dy[...]).astype(bf16).reshape(dwd.shape[1:])

    @pl.when(i < tiles)
    def _():
        slot = lax.rem(i, 2)
        load(i, lambda cp: cp.wait())
        wg, wu, wd = tg[slot].reshape(-1, TN), tu[slot].reshape(-1, TN), td[slot].reshape(TN, -1)
        for rows in chunks(tokens, MC):
            g = dot(a[rows, :], wg)
            u = dot(a[rows, :], wu)
            d = dot_nt(dy[rows, :], wd).astype(bf16).astype(f32)
            sig = jax.nn.sigmoid(g)
            silu = g * sig
            pbuf[rows, :] = (silu * u).astype(bf16)
            du[rows, :] = (d * silu).astype(bf16)
            dg[rows, :] = (d * u * (sig * (1 + g * (1 - sig)))).astype(bf16)
        for rows in chunks(tokens, MC):
            accg[rows, :] = jnp.where(i == 0, 0.0, accg[rows, :]) + dot_nt(dg[rows, :], wg)
            accu[rows, :] = jnp.where(i == 0, 0.0, accu[rows, :]) + dot_nt(du[rows, :], wu)
        by_weights(pbuf)

    @pl.when((i >= tiles) & (i < total))
    def _():
        load0(i, lambda cp: cp.wait())
        slot = lax.rem(i, 2)
        wd = td[slot].reshape(TN, -1)
        for rows in chunks(tokens, MC):
            d = dot_nt(dy[rows, :], wd).astype(bf16).astype(f32)
            du[rows, :] = (d * sv[slot, rows, :]).astype(bf16)
            dg[rows, :] = (d * tv[slot, rows, :]).astype(bf16)
        by_weights(pv.at[slot])

    @pl.when(i == tiles - 1)
    def _():
        pltpu.make_async_copy(h_ref, a, lsem.at[0]).start()

    def spread(tile):
        layer, j = 1 - tile // tiles, lax.rem(tile, tiles)
        src, dst = fin.at[tile], sums_ref.at[layer, place.y, place.z, j]
        pltpu.make_async_copy(src, dst, agr.at[0]).start()

        def one(d, _):
            to = lax.rem(r + d, 16)
            remote(src, dst, ags.at[0], agr.at[0], (0, to, place.s)).start()
            return 0

        lax.fori_loop(1, 16, one, 0)

    def first_half(tile):
        slot = lax.rem(tile, 8)
        for k, dim in enumerate("yz"):

            @pl.when(lax.rem(tile, 2) == k)
            def _(k=k, dim=dim):
                me = where[dim]
                for q in range(3):
                    held[slot, me, q] = fin[tile, q]
                for d in (1, 2, 3):
                    remote(fin.at[tile], held.at[slot, me], hs.at[k], hr.at[slot], place.along(dim, d)).start()

    def passed_on(tile):
        pltpu.make_async_copy(held.at[0], held.at[0], hs.at[2 + lax.rem(tile, 2)]).wait()
        pltpu.make_async_copy(held.at[pl.ds(0, 3)], held.at[pl.ds(0, 3)], hs.at[4 + lax.rem(tile, 2)]).wait()

    def second_half(tile):
        layer, j, slot = 1 - tile // tiles, lax.rem(tile, tiles), lax.rem(tile, 8)
        three = held.at[slot, pl.ds(0, 3)]
        pltpu.make_async_copy(three, three, hr.at[slot]).wait()
        pltpu.make_async_copy(three, three, hs.at[lax.rem(tile, 2)]).wait()

        @pl.when(tile > 1)
        def _():
            passed_on(tile - 2)

        for k, dim in enumerate("yz"):

            @pl.when(lax.rem(tile, 2) == k)
            def _(k=k, dim=dim):
                other = "z" if dim == "y" else "y"
                dst = sums_ref.at[layer, :, place.z, j] if dim == "y" else sums_ref.at[layer, place.y, :, j]
                pltpu.make_async_copy(held.at[slot], dst, hs.at[2 + k]).start()
                for d in (1, 2, 3):
                    remote(held.at[slot], dst, hs.at[4 + k], agr.at[0], place.along(other, d)).start()

    def stage4(tile):
        arrived(2, tile)
        for q in range(3):
            fin[tile, q] = added(2, tile, q)

        @pl.when(tile < total - 2)
        def _():
            first_half(tile)

        @pl.when(tile >= total - 2)
        def _():
            spread(tile)

    def stage3(tile):
        arrived(1, tile)
        for q in range(3):
            s3[lax.rem(tile, 2), q] = added(1, tile, q)
        exchange(2, tile)

    def stage2(tile):
        arrived(0, tile)
        for q in range(3):
            s2[lax.rem(tile, 2), q] = added(0, tile, q)
        exchange(1, tile)

    for stage, lag in ((stage4, 5), (stage3, 4), (stage2, 3)):
        end = total + lag - 1

        def steps(first, stage=stage, lag=lag, end=end):
            count = jnp.where(first == end - 1, 2, 1)

            def one(n, _):
                stage(first - lag + n)
                return 0

            lax.fori_loop(0, count, one, 0)

        @pl.when((i >= lag) & (i < end))
        def _(steps=steps):
            steps(i)

    @pl.when((i >= 1) & (i < total + 1))
    def _():
        tile = i - 1
        slot = lax.rem(tile, 2)
        for cp in stage0(tile):
            cp.wait()
        for xi in range(4):
            for k in range(8):
                for h in range(2):
                    rows, cols = pl.ds(16 * k, 16), pl.ds(U * h, U)
                    yi, zi = k // 2, 2 * (k % 2) + h
                    for q, at_ in ((0, (yi, zi, xi)), (1, (zi, xi, yi))):
                        v = dgu[slot, q, xi, c, rows, cols].astype(f32) + r0gu[slot, q, xi, rows, cols].astype(f32)
                        s1[(slot, q, *at_)] = v.astype(bf16)
                    rows, cols = pl.ds(16 * (yi // 2), 16), pl.ds(U * (4 * (yi % 2) + zi), U)
                    v = dwd[slot, xi, c, rows, cols].astype(f32) + r0wd[slot, xi, rows, cols].astype(f32)
                    s1[slot, 2, xi, yi, zi] = v.astype(bf16)
        exchange(0, tile)

    @pl.when(i < total)
    def _():
        for cp in stage0(i):
            cp.start()

    @pl.when(i == 0)
    def _():
        for tile in range(early + 1, tiles):
            fetch.a(tile, tile - early)

    @pl.when((i + 3 >= early) & (i + 3 < tiles))
    def _():
        fetch.d(i + 3, i + 3 - early)

    @pl.when((i + 4 >= early) & (i + 4 < tiles))
    def _():
        fetch.b(i + 4, i + 4 - early)

    @pl.when((i >= 6) & (i < total + 4))
    def _():
        second_half(i - 6)

    @pl.when(i == tiles - 1)
    def _():
        pltpu.make_async_copy(h_ref, a, lsem.at[0]).wait()
        new_at = pltpu.make_async_copy(at_ref, at, lsem.at[1])
        new_at.start()

        def some(k, _):
            rows = pl.ds(pl.multiple_of(32 * k, 32), 32)
            da = (accg[rows, :].astype(bf16) + accu[rows, :].astype(bf16)).astype(f32)
            wide = a[rows, :].astype(f32)
            scale = lax.rsqrt(jnp.mean(wide**2, -1, keepdims=True) + 1e-6)
            along = jnp.sum(da * wide, -1, keepdims=True)
            by_h = da * scale - wide * (along * (scale * scale * scale) * (1.0 / wide.shape[-1]))
            dy[rows, :] = dy[rows, :] + by_h.astype(bf16)
            return 0

        lax.fori_loop(0, tokens // 32, some, 0, unroll=4)
        new_at.wait()

    @pl.when(i == total + 3)
    def _():
        fetch.sent(tiles - early)
        passed_on(total - 4)
        passed_on(total - 3)
        for units, sem in ((2 * 15 * 3, ags.at[0]), ((total - 2) * 36 + 2 * 48, agr.at[0])):
            some = some_ref.at[pl.ds(0, units // 4)] if units % 4 == 0 else some_ref.at[pl.ds(0, units // 2), pl.ds(0, 16)]
            pltpu.make_async_copy(some, some, sem).wait()


def backward(at, h, dy, wg, wu, wd, s, t, p, early):
    tokens, d = h.shape
    ff = s.shape[1]
    tiles = ff // TN
    anywhere = pl.BlockSpec(memory_space=pl.ANY)
    dma = pltpu.SemaphoreType.DMA
    unit = (16, U)
    return pl.pallas_call(
        functools.partial(backward_kernel, tiles, early),
        grid=(2 * tiles + 4,),
        in_specs=[anywhere] * 9,
        out_specs=[anywhere] * 5,
        out_shape=[
            jax.ShapeDtypeStruct((2, 4, 4, tiles, 3, *unit), bf16),
            jax.ShapeDtypeStruct((tiles - early, 4, 2, 128, TN), bf16),
            jax.ShapeDtypeStruct((tiles - early, 4, 2, 128, TN), bf16),
            jax.ShapeDtypeStruct((tiles - early, 4, 2, 32, d), bf16),
            jax.ShapeDtypeStruct((240, 32, TN), bf16),
        ],
        scratch_shapes=[
            pltpu.VMEM((tokens, d), bf16),
            pltpu.VMEM((d, tokens), bf16),
            pltpu.VMEM((tokens, d), bf16),
            pltpu.VMEM((tokens, d), f32),
            pltpu.VMEM((tokens, d), f32),
            pltpu.VMEM((tokens, TN), bf16),
            pltpu.VMEM((tokens, TN), bf16),
            pltpu.VMEM((tokens, TN), bf16),
            pltpu.VMEM((2, 4, 2, 128, TN), bf16),
            pltpu.VMEM((2, 4, 2, 128, TN), bf16),
            pltpu.VMEM((2, 4, 2, 32, d), bf16),
            pltpu.VMEM((2, tokens, TN), f32),
            pltpu.VMEM((2, tokens, TN), f32),
            pltpu.VMEM((2, tokens, TN), bf16),
            pltpu.VMEM((2, 2, 4, 2, 128, TN), bf16),
            pltpu.VMEM((2, 4, 2, 32, d), bf16),
            pltpu.VMEM((2, 2, 4, 128, TN), bf16),
            pltpu.VMEM((2, 4, 32, d), bf16),
            pltpu.VMEM((2, 3, 4, 4, 4, *unit), bf16),
            pltpu.VMEM((4, 3, 3, 4, 4, *unit), bf16),
            pltpu.VMEM((2, 3, 4, 4, *unit), bf16),
            pltpu.VMEM((4, 3, 3, 4, *unit), bf16),
            pltpu.VMEM((2, 3, 4, *unit), bf16),
            pltpu.VMEM((4, 3, 3, *unit), bf16),
            pltpu.VMEM((2 * tiles, 3, *unit), bf16),
            pltpu.VMEM((8, 4, 3, *unit), bf16),
            dma((10,)),
            dma((2, 3, 4)),
            dma((2, 3)),
            dma((2, 2)),
            dma((2, 2)),
            dma((2,)),
            dma((4,)),
            dma((2,)),
            dma((4,)),
            dma((2,)),
            dma((4,)),
            dma((1,)),
            dma((1,)),
            dma((6,)),
            dma((8,)),
            dma((3,)),
            dma((tiles - early,)),
            dma((tiles - early,)),
            dma((tiles - early,)),
        ],
        compiler_params=pltpu.CompilerParams(vmem_limit_bytes=VMEM_LIMIT, has_side_effects=True, collective_id=2),
        cost_estimate=pl.CostEstimate(flops=24 * tokens * d * ff, bytes_accessed=10 * tokens * ff, transcendentals=0),
        name="backward",
    )(at, h, dy, wg, wu, wd, s, t, p)[0]


def adamw(w, m, v, g):
    m = 0.9 * m + 0.1 * g
    v = 0.95 * v + 0.05 * g * g
    step = m * lax.rsqrt(v + 1e-8) + 0.1 * w
    return (w - 0.02 * step).astype(bf16), m, v


ROWS = 64


def update_kernel(tiles, steps, sgu_ref, sd_ref, *refs):
    ins, outs = refs[:9], refs[9:]
    i = pl.program_id(0)

    def one(q, at_, g):
        new = adamw(ins[q][at_].astype(f32), ins[3 + q][at_], ins[6 + q][at_], g.astype(f32))
        for n, value in enumerate(new):
            outs[3 * n + q][at_] = value

    @pl.when(i < steps)
    def _():
        def some(t, _):
            rows = pl.ds(pl.multiple_of(16 * t, 16), 16)
            for q in range(2):
                for n in range(2 * tiles):
                    parts = []
                    for k in range(4 * n, 4 * n + 4):
                        owner, j = k // tiles, k % tiles
                        parts.append(sgu_ref[0, 2 * t + owner // 4, j, q, :, 32 * (owner % 4) : 32 * (owner % 4) + 32])
                    one(q, (0, rows, pl.ds(U * n, U)), jnp.concatenate(parts, axis=1))
            return 0

        lax.fori_loop(0, ROWS // 16, some, 0)

    @pl.when(i >= steps)
    def _():
        def tile(j, _):
            for k in range(2):
                for h in range(8):
                    at_ = (0, pl.ds(pl.multiple_of(32 * j + 16 * k, 16), 16), pl.ds(U * h, U))
                    one(2, at_, sd_ref[0, 8 * k + h, j, 0])
            return 0

        lax.fori_loop(0, tiles, tile, 0)


def update(sums, weights, m, v):
    layers, rows, ff = weights[0].shape
    tiles = ff // TN
    each = rows // ROWS
    steps = layers * each
    here = lambda i: (jnp.minimum(i, steps - 1) // each, jnp.minimum(i, steps - 1) % each)
    gu = pl.BlockSpec((1, ROWS, ff), lambda i: (*here(i), 0))
    down = lambda i: jnp.maximum(i - steps, 0)
    wd = pl.BlockSpec((1, *weights[2].shape[1:]), lambda i: (down(i), 0, 0))
    specs = [gu, gu, wd] * 3
    arrays = (*weights, *m, *v)
    return pl.pallas_call(
        functools.partial(update_kernel, tiles, steps),
        grid=(steps + layers,),
        in_specs=[
            pl.BlockSpec((1, ROWS // 8, tiles, 3, 16, U), lambda i: (*here(i), 0, 0, 0, 0)),
            pl.BlockSpec((1, 16, tiles, 1, 16, U), lambda i: (down(i), 0, 0, 2, 0, 0)),
        ]
        + specs,
        out_specs=specs,
        out_shape=[jax.ShapeDtypeStruct(one.shape, one.dtype) for one in arrays],
        compiler_params=pltpu.CompilerParams(vmem_limit_bytes=VMEM_LIMIT),
        name="update",
    )(sums, sums, *arrays)


def solution(mesh):
    def step(x, dy, *arrays):
        weights, m, v = (arrays[i : i + 3] for i in (0, 3, 6))
        early = 4
        s, t, p, h, at, *whole, _ = forward(x[0], *weights, early)
        sums = backward(at, h, dy[0], *whole, s, t, p, early)
        sums = sums.reshape(2, 16, *sums.shape[3:])
        return tuple(update(sums, weights, m, v))

    states, cut = P(("rep", "r", "s"), None, None), P(None, "s", None)
    return jax.shard_map(
        step,
        mesh=mesh,
        in_specs=(states, states) + (cut,) * 9,
        out_specs=(P("rep", "s", None),) * 9,
        check_vma=False,
    )
```

```python
import functools

import jax
import jax.numpy as jnp
from jax import lax
from jax.experimental import pallas as pl
from jax.experimental.pallas import tpu as pltpu
from jax.sharding import PartitionSpec as P

MESH = pl.DeviceIdType.MESH
f32, bf16 = jnp.float32, jnp.bfloat16
TN = 256
MC = 512
U = 128
VMEM_LIMIT = 67043328


def dot(a, b):
    return lax.dot_general(a, b, (((1,), (0,)), ((), ())), preferred_element_type=f32)


def dot_nt(a, b):
    return lax.dot_general(a, b, (((1,), (1,)), ((), ())), preferred_element_type=f32)


def normed(h):
    wide = h.astype(f32)
    scale = lax.rsqrt(jnp.mean(wide**2, -1, keepdims=True) + 1e-6)
    return (wide * scale).astype(bf16)


def chunks(n, step):
    return [pl.ds(i, step) for i in range(0, n, step)]


class Place:
    def __init__(self):
        self.r, self.s = lax.axis_index("r"), lax.axis_index("s")
        self.y, self.z, self.x, self.c = self.r // 4, self.r % 4, self.s // 2, self.s % 2
        self.peer = (0, self.r, self.s + 1 - 2 * self.c)

    def along(self, dim, d):
        if dim == "y":
            return (0, lax.rem(self.y + d, 4) * 4 + self.z, self.s)
        if dim == "z":
            return (0, self.y * 4 + lax.rem(self.z + d, 4), self.s)
        return (0, self.r, lax.rem(self.x + d, 4) * 2 + self.c)


    def partners(self, along_r):
        some = [self.peer] + [self.along("x", d) for d in (1, 2, 3)]
        if along_r:
            return some + [(0, lax.rem(self.r + d, 16), self.s) for d in range(1, 16)]
        return some + [self.along(dim, d) for dim in "yz" for d in (1, 2, 3)]

    def greet(self, along_r=False):
        barrier = pltpu.get_barrier_semaphore()
        for one in self.partners(along_r):
            pl.semaphore_signal(barrier, inc=1, device_id=one, device_id_type=MESH)

    def greeted(self, along_r=False):
        pl.semaphore_wait(pltpu.get_barrier_semaphore(), len(self.partners(along_r)))


def remote(src, dst, ss, rs, dev):
    return pltpu.make_async_remote_copy(src_ref=src, dst_ref=dst, send_sem=ss, recv_sem=rs, device_id=dev, device_id_type=MESH)


class Fetch:
    A, B = 288, 864

    def __init__(self, place, own, whole, some, sends, recvs, first):
        self.p, self.own, self.whole, self.some, self.sends, self.recvs = place, own, whole, some, sends, recvs
        self.handed = pl.ds(first, 4 - first)
        self.D = 384 * (4 - first)

    def quarters(self, refs, *owner):
        p, (wg, wu, wd) = self.p, refs
        every = (slice(None),)
        return (
            (wg.at[(*owner, pl.ds(32 * p.y, 32))], "y"),
            (wu.at[(*owner, pl.ds(32 * p.z, 32))], "z"),
            (wd.at[(*owner, *every, pl.ds(pl.multiple_of(128 * p.y, 128), 128))], "y"),
            (wd.at[(*owner, *every, pl.ds(pl.multiple_of(512 + 128 * p.z, 128), 128))], "z"),
        )

    def wait(self, rows, sem):
        some = self.some.at[pl.ds(0, rows // 32)]
        pltpu.make_async_copy(some, some, sem).wait()

    def a(self, tile, n):
        src = self.quarters(self.own(tile))
        for d in (1, 2, 3):
            dst = self.quarters(self.whole(tile), 4 - d, self.p.c)
            for (one, _), (other, _) in zip(src, dst, strict=True):
                remote(one, other, self.sends.at[0], self.recvs[0].at[n], self.p.along("x", d)).start()

    def b(self, tile, n):
        self.wait(self.A, self.recvs[0].at[n])
        for ref, dim in self.quarters(self.whole(tile), pl.ds(1, 3), self.p.c):
            for d in (1, 2, 3):
                remote(ref, ref, self.sends.at[1], self.recvs[1].at[n], self.p.along(dim, d)).start()

    def d(self, tile, n):
        self.wait(self.B, self.recvs[1].at[n])
        for whole in self.whole(tile):
            ref = whole.at[self.handed, self.p.c]
            remote(ref, ref, self.sends.at[2], self.recvs[2].at[n], self.p.peer).start()

    def here(self, n):
        self.wait(self.D, self.recvs[2].at[n])

    def sent(self, count):
        def one(_n, _):
            for k, rows in enumerate((self.A, self.B, self.D)):
                self.wait(rows, self.sends.at[k])
            return 0

        lax.fori_loop(0, count, one, 0)


def forward_kernel(tiles, early, x_ref, wg_ref, wu_ref, wd_ref, s_out, t_out, p_out, h_ref, at_ref, wg_all, wu_all, wd_all, some_ref,
                   xv, wg_in, wu_in, wd_in, a, at, acc, wgp, wup, tg, tu, td, sv, tv, pv, ksem, isem, osem, orecv, lsem, sends, arecv, brecv, drecv):
    k = pl.program_id(0)
    tokens = x_ref.shape[0]
    place = Place()
    count = tiles + early
    fetch = Fetch(
        place,
        lambda n: (wgp.at[n // tiles, lax.rem(n, tiles)], wup.at[n // tiles, lax.rem(n, tiles)], wd_in.at[n // tiles, lax.rem(n, tiles)]),
        lambda n: (wg_all.at[n // tiles, lax.rem(n, tiles)], wu_all.at[n // tiles, lax.rem(n, tiles)], wd_all.at[n // tiles, lax.rem(n, tiles)]),
        some_ref,
        sends,
        (arecv, brecv, drecv),
        0,
    )

    def own_copies(n):
        blocks = ((wgp.at[n], wg_all.at[n, :, 0, place.c]), (wup.at[n], wu_all.at[n, :, 0, place.c]), (wd_in.at[n], wd_all.at[n, :, 0, place.c]))
        copies = [pltpu.make_async_copy(src, dst, lsem.at[n, m, 0]) for m, (src, dst) in enumerate(blocks)]
        if n == 1:
            late = pl.ds(early, tiles - early)
            copies += [remote(src.at[late], dst.at[late], osem.at[m], orecv.at[m], place.peer) for m, (src, dst) in enumerate(blocks)]
        return copies

    quarter = lax.broadcasted_iota(jnp.int32, (16, U), 1) // 32

    def permute(n):
        def rows_of(i, _):
            rows = pl.ds(pl.multiple_of(16 * i, 16), 16)
            for src, dst in ((wg_in, wgp), (wu_in, wup)):
                for j in range(tiles):
                    for h in range(2):
                        v = None
                        for o in range(4 * h, 4 * h + 4):
                            one = src[n, rows, pl.ds((416 * o + 32 * j) // U * U, U)]
                            v = one if v is None else jnp.where(quarter == (o + j) % 4, one, v)
                        t = 32 * (j % 4)
                        if t:
                            v = jnp.concatenate([v[:, t:], v[:, :t]], axis=1)
                        dst[n, j, rows, U * h : U * h + U] = v
            return 0

        lax.fori_loop(0, 8, rows_of, 0)

    def loads(tile):
        slot = lax.rem(tile, 2)
        copies = []
        for q, (src, dst) in enumerate(((wg_all, tg), (wu_all, tu), (wd_all, td))):
            for e in range(4):
                copies.append(pltpu.make_async_copy(src.at[0, tile, e], dst.at[slot, lax.rem(place.x + e, 4)], lsem.at[2 + slot, q, e]))
        return copies

    def load(tile):
        fetch.here(tile)
        for cp in loads(tile):
            cp.start()

    def fetched(n):
        pairs = ((wg_ref, wg_in), (wu_ref, wu_in), (wd_ref, wd_in))
        return [pltpu.make_async_copy(src.at[n], dst.at[n], isem.at[13 * n + m]) for m, (src, dst) in enumerate(pairs)]

    def out_at():
        return pltpu.make_async_copy(at, at_ref, isem.at[4])

    @pl.when(k == 0)
    def _():
        place.greet()
        for cp in fetched(0):
            cp.start()
        get_x = pltpu.make_async_copy(x_ref, xv, isem.at[3])
        get_x.start()
        for cp in fetched(1):
            cp.start()
        for cp in fetched(0):
            cp.wait()
        permute(0)
        place.greeted()
        for n in range(3):
            fetch.a(n, n)
        for cp in own_copies(0):
            cp.start()
        for n in range(3, 5):
            fetch.a(n, n)
        get_x.wait()
        for rows in chunks(tokens, 256):
            a[rows, :] = normed(xv[rows, :])
        fetch.b(0, 0)
        fetch.b(1, 1)
        for rows in chunks(tokens, 256):
            at[:, rows] = a[rows, :].T
        out_at().start()
        for cp in own_copies(0):
            cp.wait()
        fetch.d(0, 0)
        fetch.b(2, 2)
        fetch.b(3, 3)
        load(0)

    @pl.when((k >= 2) & (k < tiles - 1))
    def _():
        load(k + 1)

    def ahead(stage, lead, more):
        @pl.when((k >= 2) & (k <= more))
        def _():
            stage(k + lead, k + lead)

        @pl.when((k >= more) & (k + lead + 1 < count))
        def _():
            stage(k + lead + 1, k + lead + 1)

    ahead(fetch.a, 5, 6)
    ahead(fetch.b, 4, 8)
    ahead(fetch.d, 2, 10)

    slot = lax.rem(k, 2)
    for cp in loads(k):
        cp.wait()
    def keep(tile):
        slot = lax.rem(tile, 2)
        cols = pl.ds(pl.multiple_of(TN * tile, TN), TN)
        pairs = ((sv, s_out), (tv, t_out), (pv, p_out))
        return [pltpu.make_async_copy(src.at[slot], dst.at[:, cols], ksem.at[slot, q]) for q, (src, dst) in enumerate(pairs)]

    @pl.when(k >= 2)
    def _():
        for cp in keep(k - 2):
            cp.wait()

    wg, wu, wd = tg[slot].reshape(-1, TN), tu[slot].reshape(-1, TN), td[slot].reshape(TN, -1)
    for rows in chunks(tokens, MC):
        g = dot(a[rows, :], wg)
        u = dot(a[rows, :], wu)
        sig = jax.nn.sigmoid(g)
        silu = g * sig
        sv[slot, rows, :] = silu
        tv[slot, rows, :] = u * (sig * (1 + g * (1 - sig)))
        pv[slot, rows, :] = (silu * u).astype(bf16)
    for rows in chunks(tokens, MC):
        acc[rows, :] = jnp.where(k == 0, 0.0, acc[rows, :]) + dot(pv[slot, rows, :], wd)
    for cp in keep(k):
        cp.start()

    @pl.when(k == 0)
    def _():
        fetch.d(1, 1)
        fetch.b(4, 4)
        fetch.a(5, 5)
        fetch.d(2, 2)
        load(1)

    @pl.when(k == 1)
    def _():
        fetch.d(3, 3)
        load(2)
        fetch.b(5, 5)
        fetch.a(6, 6)

    @pl.when(k == 2)
    def _():
        for cp in fetched(1):
            cp.wait()
        permute(1)

    @pl.when(k == 6)
    def _():
        for cp in own_copies(1):
            cp.start()

    @pl.when(k == 8)
    def _():
        for cp in own_copies(1):
            cp.wait()

    @pl.when(k == tiles - 1)
    def _():
        fetch.d(count - 1, count - 1)
        parts = chunks(tokens, 256)
        out_h = [pltpu.make_async_copy(xv.at[rows, :], h_ref.at[rows, :], isem.at[5 + m]) for m, rows in enumerate(parts)]
        for rows, cp in zip(parts, out_h, strict=True):
            xv[rows, :] = xv[rows, :] + acc[rows, :].astype(bf16)
            cp.start()
        for n in range(tiles, count):
            fetch.here(n)
        fetch.sent(count)
        out_at().wait()
        for cp in out_h + keep(k - 1) + keep(k):
            cp.wait()


def forward(x, wg, wu, wd, early):
    tokens, d = x.shape
    ff = wg.shape[2]
    tiles = ff // TN
    assert early == 4
    anywhere = pl.BlockSpec(memory_space=pl.ANY)
    wd = wd.reshape(2, tiles, 32, d)
    dma = pltpu.SemaphoreType.DMA
    return pl.pallas_call(
        functools.partial(forward_kernel, tiles, early),
        grid=(tiles,),
        in_specs=[anywhere] * 4,
        out_specs=[anywhere] * 9,
        out_shape=[jax.ShapeDtypeStruct((tokens, ff), f32)] * 2
        + [jax.ShapeDtypeStruct((tokens, ff), bf16), jax.ShapeDtypeStruct((tokens, d), bf16), jax.ShapeDtypeStruct((d, tokens), bf16)]
        + [jax.ShapeDtypeStruct((2, tiles, 4, 2, 128, TN), bf16)] * 2
        + [jax.ShapeDtypeStruct((2, tiles, 4, 2, 32, d), bf16)]
        + [jax.ShapeDtypeStruct((48, 32, TN), bf16)],
        scratch_shapes=[
            pltpu.VMEM((tokens, d), bf16),
            pltpu.VMEM(wg.shape, bf16),
            pltpu.VMEM(wu.shape, bf16),
            pltpu.VMEM(wd.shape, bf16),
            pltpu.VMEM((tokens, d), bf16),
            pltpu.VMEM((d, tokens), bf16),
            pltpu.VMEM((tokens, d), f32),
            pltpu.VMEM((2, tiles, 128, TN), bf16),
            pltpu.VMEM((2, tiles, 128, TN), bf16),
            pltpu.VMEM((2, 4, 2, 128, TN), bf16),
            pltpu.VMEM((2, 4, 2, 128, TN), bf16),
            pltpu.VMEM((2, 4, 2, 32, d), bf16),
            pltpu.VMEM((2, tokens, TN), f32),
            pltpu.VMEM((2, tokens, TN), f32),
            pltpu.VMEM((2, tokens, TN), bf16),
            dma((2, 3)),
            dma((16,)),
            dma((3,)),
            dma((3,)),
            dma((4, 3, 4)),
            dma((3,)),
            dma((tiles + early,)),
            dma((tiles + early,)),
            dma((tiles + early,)),
        ],
        compiler_params=pltpu.CompilerParams(vmem_limit_bytes=VMEM_LIMIT, has_side_effects=True, collective_id=1),
        cost_estimate=pl.CostEstimate(flops=6 * tokens * d * ff, bytes_accessed=10 * tokens * ff, transcendentals=0),
        name="forward0",
    )(x, wg, wu, wd)


def backward_kernel(tiles, early, at_ref, h_ref, dy_ref, wg_ref, wu_ref, wd_ref, s_ref, t_ref, p_ref,
                    sums_ref, wg_more, wu_more, wd_more, some_ref,
                    a, at, dy, accg, accu, pbuf, dg, du, tg, tu, td, sv, tv, pv, dgu, dwd, r0gu, r0wd, s1, r1, s2, r2, s3, r3, fin, held,
                    lsem, tsem, hsem, s0s, s0r, s1s, s1r, s2s, s2r, s3s, s3r, ags, agr, hs, hr, sends, arecv, brecv, drecv):
    i = pl.program_id(0)
    tokens = a.shape[0]
    place = Place()
    r, c = place.r, place.c
    total = 2 * tiles
    where = {"x": place.x, "y": place.y, "z": place.z}
    ORDER = ("yzx", "zxy", "xyz")

    def stage0(tile):
        slot = lax.rem(tile, 2)
        return [
            remote(dgu.at[slot, :, :, 1 - c], r0gu.at[slot], s0s.at[slot, 0], s0r.at[slot, 0], place.peer),
            remote(dwd.at[slot, :, 1 - c], r0wd.at[slot], s0s.at[slot, 1], s0r.at[slot, 1], place.peer),
        ]

    STAGES = ((s1, r1, s1s, s1r, 2, 4), (s2, r2, s2s, s2r, 2, 4), (s3, r3, s3s, s3r, 2, 4))

    def exchange(n, tile):
        src, dst, ss, rs, held, slots = STAGES[n]
        own, slot = lax.rem(tile, held), lax.rem(tile, slots)
        for q in range(3):
            dim = ORDER[q][n]
            for d in (1, 2, 3):
                part = src.at[own, q, lax.rem(where[dim] + d, 4)]
                remote(part, dst.at[slot, q, d - 1], ss.at[own], rs.at[slot], place.along(dim, d)).start()

    def arrived(n, tile):
        src, dst, ss, rs, held, slots = STAGES[n]
        own, slot = lax.rem(tile, held), lax.rem(tile, slots)
        sent = src.at[own, :, pl.ds(0, 3)]
        pltpu.make_async_copy(sent, sent, ss.at[own]).wait()
        pltpu.make_async_copy(dst.at[slot], dst.at[slot], rs.at[slot]).wait()

    def added(n, tile, q):
        src, dst, _ss, _rs, held, slots = STAGES[n]
        slot = lax.rem(tile, slots)
        own = src[lax.rem(tile, held), q, where[ORDER[q][n]]].astype(f32)
        return (own + dst[slot, q, 0].astype(f32) + dst[slot, q, 1].astype(f32) + dst[slot, q, 2].astype(f32)).astype(bf16)

    fetch = Fetch(
        place,
        lambda j: tuple(w.at[1, j, 0, place.c] for w in (wg_ref, wu_ref, wd_ref)),
        lambda j: (wg_more.at[j - early], wu_more.at[j - early], wd_more.at[j - early]),
        some_ref,
        sends,
        (arecv, brecv, drecv),
        1,
    )

    def load(tile, act):
        slot = lax.rem(tile, 2)
        for own, some in ((tile < early, lambda w, _more, e: w.at[1, tile, e]), (tile >= early, lambda w, more, e: more.at[tile - early, e] if e else w.at[1, tile, e])):

            @pl.when(own)
            def _(some=some):
                for q, (w, more, dst) in enumerate(((wg_ref, wg_more, tg), (wu_ref, wu_more, tu), (wd_ref, wd_more, td))):
                    for e in range(4):
                        act(pltpu.make_async_copy(some(w, more, e), dst.at[slot, lax.rem(place.x + e, 4)], tsem.at[slot, q, e]))

    def load0(tile, act):
        slot = lax.rem(tile, 2)
        for e in range(4):
            act(pltpu.make_async_copy(wd_ref.at[0, tile - tiles, e], td.at[slot, lax.rem(place.x + e, 4)], tsem.at[slot, 2, e]))
        cols = pl.ds(pl.multiple_of(TN * (tile - tiles), TN), TN)
        for q, (src, dst) in enumerate(((s_ref, sv), (t_ref, tv), (p_ref, pv))):
            act(pltpu.make_async_copy(src.at[:, cols], dst.at[slot], hsem.at[slot, q]))

    @pl.when(i == 0)
    def _():
        place.greet(True)
        parts = chunks(tokens, 256)
        copies = [pltpu.make_async_copy(h_ref.at[rows, :], a.at[rows, :], lsem.at[2 + n]) for n, rows in enumerate(parts)]
        for cp in copies:
            cp.start()
        get_dy = pltpu.make_async_copy(dy_ref, dy, lsem.at[1])
        get_dy.start()
        load(i, lambda cp: cp.start())
        for rows, cp in zip(parts, copies, strict=True):
            cp.wait()
            v = normed(a[rows, :])
            a[rows, :] = v
            at[:, rows] = v.T
        get_dy.wait()
        place.greeted(True)
        fetch.a(early, 0)

    @pl.when((i >= early - 1) & (i < tiles - 1))
    def _():
        fetch.here(i + 1 - early)

    @pl.when(i < tiles - 1)
    def _():
        load(i + 1, lambda cp: cp.start())

    @pl.when((i >= tiles - 1) & (i < total - 1))
    def _():
        load0(i + 1, lambda cp: cp.start())

    def by_weights(p):
        slot = lax.rem(i, 2)
        for q, one in ((0, dg), (1, du)):
            dgu[slot, q] = dot(at[...], one[...]).astype(bf16).reshape(dgu.shape[2:])
        dwd[slot] = dot(p[...].T, dy[...]).astype(bf16).reshape(dwd.shape[1:])

    @pl.when(i < tiles)
    def _():
        slot = lax.rem(i, 2)
        load(i, lambda cp: cp.wait())
        wg, wu, wd = tg[slot].reshape(-1, TN), tu[slot].reshape(-1, TN), td[slot].reshape(TN, -1)
        for rows in chunks(tokens, MC):
            g = dot(a[rows, :], wg)
            u = dot(a[rows, :], wu)
            d = dot_nt(dy[rows, :], wd).astype(bf16).astype(f32)
            sig = jax.nn.sigmoid(g)
            silu = g * sig
            pbuf[rows, :] = (silu * u).astype(bf16)
            du[rows, :] = (d * silu).astype(bf16)
            dg[rows, :] = (d * u * (sig * (1 + g * (1 - sig)))).astype(bf16)
        for rows in chunks(tokens, MC):
            accg[rows, :] = jnp.where(i == 0, 0.0, accg[rows, :]) + dot_nt(dg[rows, :], wg)
            accu[rows, :] = jnp.where(i == 0, 0.0, accu[rows, :]) + dot_nt(du[rows, :], wu)
        by_weights(pbuf)

    @pl.when((i >= tiles) & (i < total))
    def _():
        load0(i, lambda cp: cp.wait())
        slot = lax.rem(i, 2)
        wd = td[slot].reshape(TN, -1)
        for rows in chunks(tokens, MC):
            d = dot_nt(dy[rows, :], wd).astype(bf16).astype(f32)
            du[rows, :] = (d * sv[slot, rows, :]).astype(bf16)
            dg[rows, :] = (d * tv[slot, rows, :]).astype(bf16)
        by_weights(pv.at[slot])

    @pl.when(i == tiles - 1)
    def _():
        pltpu.make_async_copy(h_ref, a, lsem.at[0]).start()

    def spread(tile):
        layer, j = 1 - tile // tiles, lax.rem(tile, tiles)
        src, dst = fin.at[tile], sums_ref.at[layer, place.y, place.z, j]
        pltpu.make_async_copy(src, dst, agr.at[0]).start()

        def one(d, _):
            to = lax.rem(r + d, 16)
            remote(src, dst, ags.at[0], agr.at[0], (0, to, place.s)).start()
            return 0

        lax.fori_loop(1, 16, one, 0)

    def first_half(tile):
        slot = lax.rem(tile, 8)
        for k, dim in enumerate("yz"):

            @pl.when(lax.rem(tile, 2) == k)
            def _(k=k, dim=dim):
                me = where[dim]
                for q in range(3):
                    held[slot, me, q] = fin[tile, q]
                for d in (1, 2, 3):
                    remote(fin.at[tile], held.at[slot, me], hs.at[k], hr.at[slot], place.along(dim, d)).start()

    def passed_on(tile):
        pltpu.make_async_copy(held.at[0], held.at[0], hs.at[2 + lax.rem(tile, 2)]).wait()
        pltpu.make_async_copy(held.at[pl.ds(0, 3)], held.at[pl.ds(0, 3)], hs.at[4 + lax.rem(tile, 2)]).wait()

    def second_half(tile):
        layer, j, slot = 1 - tile // tiles, lax.rem(tile, tiles), lax.rem(tile, 8)
        three = held.at[slot, pl.ds(0, 3)]
        pltpu.make_async_copy(three, three, hr.at[slot]).wait()
        pltpu.make_async_copy(three, three, hs.at[lax.rem(tile, 2)]).wait()

        @pl.when(tile > 1)
        def _():
            passed_on(tile - 2)

        for k, dim in enumerate("yz"):

            @pl.when(lax.rem(tile, 2) == k)
            def _(k=k, dim=dim):
                other = "z" if dim == "y" else "y"
                dst = sums_ref.at[layer, :, place.z, j] if dim == "y" else sums_ref.at[layer, place.y, :, j]
                pltpu.make_async_copy(held.at[slot], dst, hs.at[2 + k]).start()
                for d in (1, 2, 3):
                    remote(held.at[slot], dst, hs.at[4 + k], agr.at[0], place.along(other, d)).start()

    def stage4(tile):
        arrived(2, tile)
        for q in range(3):
            fin[tile, q] = added(2, tile, q)

        @pl.when(tile < total - 2)
        def _():
            first_half(tile)

        @pl.when(tile >= total - 2)
        def _():
            spread(tile)

    def stage3(tile):
        arrived(1, tile)
        for q in range(3):
            s3[lax.rem(tile, 2), q] = added(1, tile, q)
        exchange(2, tile)

    def stage2(tile):
        arrived(0, tile)
        for q in range(3):
            s2[lax.rem(tile, 2), q] = added(0, tile, q)
        exchange(1, tile)

    for stage, lag in ((stage4, 5), (stage3, 4), (stage2, 3)):
        end = total + lag - 1

        def steps(first, stage=stage, lag=lag, end=end):
            count = jnp.where(first == end - 1, 2, 1)

            def one(n, _):
                stage(first - lag + n)
                return 0

            lax.fori_loop(0, count, one, 0)

        @pl.when((i >= lag) & (i < end))
        def _(steps=steps):
            steps(i)

    @pl.when((i >= 1) & (i < total + 1))
    def _():
        tile = i - 1
        slot = lax.rem(tile, 2)
        for cp in stage0(tile):
            cp.wait()
        for xi in range(4):
            for k in range(8):
                for h in range(2):
                    rows, cols = pl.ds(16 * k, 16), pl.ds(U * h, U)
                    yi, zi = k // 2, 2 * (k % 2) + h
                    for q, at_ in ((0, (yi, zi, xi)), (1, (zi, xi, yi))):
                        v = dgu[slot, q, xi, c, rows, cols].astype(f32) + r0gu[slot, q, xi, rows, cols].astype(f32)
                        s1[(slot, q, *at_)] = v.astype(bf16)
                    rows, cols = pl.ds(16 * (yi // 2), 16), pl.ds(U * (4 * (yi % 2) + zi), U)
                    v = dwd[slot, xi, c, rows, cols].astype(f32) + r0wd[slot, xi, rows, cols].astype(f32)
                    s1[slot, 2, xi, yi, zi] = v.astype(bf16)
        exchange(0, tile)

    @pl.when(i < total)
    def _():
        for cp in stage0(i):
            cp.start()

    @pl.when(i == 0)
    def _():
        for tile in range(early + 1, tiles):
            fetch.a(tile, tile - early)

    @pl.when((i + 3 >= early) & (i + 3 < tiles))
    def _():
        fetch.d(i + 3, i + 3 - early)

    @pl.when((i + 4 >= early) & (i + 4 < tiles))
    def _():
        fetch.b(i + 4, i + 4 - early)

    @pl.when((i >= 6) & (i < total + 4))
    def _():
        second_half(i - 6)

    @pl.when(i == tiles - 1)
    def _():
        pltpu.make_async_copy(h_ref, a, lsem.at[0]).wait()
        new_at = pltpu.make_async_copy(at_ref, at, lsem.at[1])
        new_at.start()

        def some(k, _):
            rows = pl.ds(pl.multiple_of(32 * k, 32), 32)
            da = (accg[rows, :].astype(bf16) + accu[rows, :].astype(bf16)).astype(f32)
            wide = a[rows, :].astype(f32)
            scale = lax.rsqrt(jnp.mean(wide**2, -1, keepdims=True) + 1e-6)
            along = jnp.sum(da * wide, -1, keepdims=True)
            by_h = da * scale - wide * (along * (scale * scale * scale) * (1.0 / wide.shape[-1]))
            dy[rows, :] = dy[rows, :] + by_h.astype(bf16)
            return 0

        lax.fori_loop(0, tokens // 32, some, 0, unroll=4)
        new_at.wait()

    @pl.when(i == total + 3)
    def _():
        fetch.sent(tiles - early)
        passed_on(total - 4)
        passed_on(total - 3)
        for units, sem in ((2 * 15 * 3, ags.at[0]), ((total - 2) * 36 + 2 * 48, agr.at[0])):
            some = some_ref.at[pl.ds(0, units // 4)] if units % 4 == 0 else some_ref.at[pl.ds(0, units // 2), pl.ds(0, 16)]
            pltpu.make_async_copy(some, some, sem).wait()


def backward(at, h, dy, wg, wu, wd, s, t, p, early):
    tokens, d = h.shape
    ff = s.shape[1]
    tiles = ff // TN
    anywhere = pl.BlockSpec(memory_space=pl.ANY)
    dma = pltpu.SemaphoreType.DMA
    unit = (16, U)
    return pl.pallas_call(
        functools.partial(backward_kernel, tiles, early),
        grid=(2 * tiles + 4,),
        in_specs=[anywhere] * 9,
        out_specs=[anywhere] * 5,
        out_shape=[
            jax.ShapeDtypeStruct((2, 4, 4, tiles, 3, *unit), bf16),
            jax.ShapeDtypeStruct((tiles - early, 4, 2, 128, TN), bf16),
            jax.ShapeDtypeStruct((tiles - early, 4, 2, 128, TN), bf16),
            jax.ShapeDtypeStruct((tiles - early, 4, 2, 32, d), bf16),
            jax.ShapeDtypeStruct((240, 32, TN), bf16),
        ],
        scratch_shapes=[
            pltpu.VMEM((tokens, d), bf16),
            pltpu.VMEM((d, tokens), bf16),
            pltpu.VMEM((tokens, d), bf16),
            pltpu.VMEM((tokens, d), f32),
            pltpu.VMEM((tokens, d), f32),
            pltpu.VMEM((tokens, TN), bf16),
            pltpu.VMEM((tokens, TN), bf16),
            pltpu.VMEM((tokens, TN), bf16),
            pltpu.VMEM((2, 4, 2, 128, TN), bf16),
            pltpu.VMEM((2, 4, 2, 128, TN), bf16),
            pltpu.VMEM((2, 4, 2, 32, d), bf16),
            pltpu.VMEM((2, tokens, TN), f32),
            pltpu.VMEM((2, tokens, TN), f32),
            pltpu.VMEM((2, tokens, TN), bf16),
            pltpu.VMEM((2, 2, 4, 2, 128, TN), bf16),
            pltpu.VMEM((2, 4, 2, 32, d), bf16),
            pltpu.VMEM((2, 2, 4, 128, TN), bf16),
            pltpu.VMEM((2, 4, 32, d), bf16),
            pltpu.VMEM((2, 3, 4, 4, 4, *unit), bf16),
            pltpu.VMEM((4, 3, 3, 4, 4, *unit), bf16),
            pltpu.VMEM((2, 3, 4, 4, *unit), bf16),
            pltpu.VMEM((4, 3, 3, 4, *unit), bf16),
            pltpu.VMEM((2, 3, 4, *unit), bf16),
            pltpu.VMEM((4, 3, 3, *unit), bf16),
            pltpu.VMEM((2 * tiles, 3, *unit), bf16),
            pltpu.VMEM((8, 4, 3, *unit), bf16),
            dma((10,)),
            dma((2, 3, 4)),
            dma((2, 3)),
            dma((2, 2)),
            dma((2, 2)),
            dma((2,)),
            dma((4,)),
            dma((2,)),
            dma((4,)),
            dma((2,)),
            dma((4,)),
            dma((1,)),
            dma((1,)),
            dma((6,)),
            dma((8,)),
            dma((3,)),
            dma((tiles - early,)),
            dma((tiles - early,)),
            dma((tiles - early,)),
        ],
        compiler_params=pltpu.CompilerParams(vmem_limit_bytes=VMEM_LIMIT, has_side_effects=True, collective_id=2),
        cost_estimate=pl.CostEstimate(flops=24 * tokens * d * ff, bytes_accessed=10 * tokens * ff, transcendentals=0),
        name="backward",
    )(at, h, dy, wg, wu, wd, s, t, p)[0]


def adamw(w, m, v, g):
    m = 0.9 * m + 0.1 * g
    v = 0.95 * v + 0.05 * g * g
    step = m * lax.rsqrt(v + 1e-8) + 0.1 * w
    return (w - 0.02 * step).astype(bf16), m, v


ROWS = 128


def update_kernel(tiles, steps, sgu_ref, sd_ref, *refs):
    ins, outs = refs[:9], refs[9:]
    i = pl.program_id(0)

    def one(q, at_, g):
        new = adamw(ins[q][at_].astype(f32), ins[3 + q][at_], ins[6 + q][at_], g.astype(f32))
        for n, value in enumerate(new):
            outs[3 * n + q][at_] = value

    @pl.when(i < steps)
    def _():
        def some(t, _):
            rows = pl.ds(pl.multiple_of(16 * t, 16), 16)
            for q in range(2):
                for n in range(2 * tiles):
                    parts = []
                    for k in range(4 * n, 4 * n + 4):
                        owner, j = k // tiles, k % tiles
                        parts.append(sgu_ref[0, 2 * t + owner // 4, j, q, :, 32 * (owner % 4) : 32 * (owner % 4) + 32])
                    one(q, (0, rows, pl.ds(U * n, U)), jnp.concatenate(parts, axis=1))
            return 0

        lax.fori_loop(0, ROWS // 16, some, 0)

    @pl.when(i >= steps)
    def _():
        def tile(j, _):
            for k in range(2):
                for h in range(8):
                    at_ = (0, pl.ds(pl.multiple_of(32 * j + 16 * k, 16), 16), pl.ds(U * h, U))
                    one(2, at_, sd_ref[0, 8 * k + h, j, 0])
            return 0

        lax.fori_loop(0, tiles, tile, 0)


def update(sums, weights, m, v):
    layers, rows, ff = weights[0].shape
    tiles = ff // TN
    each = rows // ROWS
    steps = layers * each
    here = lambda i: (jnp.minimum(i, steps - 1) // each, jnp.minimum(i, steps - 1) % each)
    gu = pl.BlockSpec((1, ROWS, ff), lambda i: (*here(i), 0))
    down = lambda i: jnp.maximum(i - steps, 0)
    wd = pl.BlockSpec((1, *weights[2].shape[1:]), lambda i: (down(i), 0, 0))
    specs = [gu, gu, wd] * 3
    arrays = (*weights, *m, *v)
    return pl.pallas_call(
        functools.partial(update_kernel, tiles, steps),
        grid=(steps + layers,),
        in_specs=[
            pl.BlockSpec((1, ROWS // 8, tiles, 3, 16, U), lambda i: (*here(i), 0, 0, 0, 0)),
            pl.BlockSpec((1, 16, tiles, 1, 16, U), lambda i: (down(i), 0, 0, 2, 0, 0)),
        ]
        + specs,
        out_specs=specs,
        out_shape=[jax.ShapeDtypeStruct(one.shape, one.dtype) for one in arrays],
        compiler_params=pltpu.CompilerParams(vmem_limit_bytes=VMEM_LIMIT),
        name="update",
    )(sums, sums, *arrays)


def solution(mesh):
    def step(x, dy, *arrays):
        weights, m, v = (arrays[i : i + 3] for i in (0, 3, 6))
        early = 4
        s, t, p, h, at, *whole, _ = forward(x[0], *weights, early)
        sums = backward(at, h, dy[0], *whole, s, t, p, early)
        sums = sums.reshape(2, 16, *sums.shape[3:])
        return tuple(update(sums, weights, m, v))

    states, cut = P(("rep", "r", "s"), None, None), P(None, "s", None)
    return jax.shard_map(
        step,
        mesh=mesh,
        in_specs=(states, states) + (cut,) * 9,
        out_specs=(P("rep", "s", None),) * 9,
        check_vma=False,
    )
```
